256 devices in a mesh: seq: 64 (over x, z_lo, y), chan: 4 (over z_hi, core).
Axes of the slice: x: 4, y: 4, z: 8 (z_hi: 2, z_lo: 4; z = z_hi * 4 + z_lo), core: 2. Of those that a mesh axis runs over, the one named last changes fastest.
Arguments:
- fwd_q: bfloat16 [8192, 4096], P('seq', 'chan'), may hold values from -6 to 6
- fwd_k: bfloat16 [8192, 4096], P('seq', 'chan'), may hold values from -6 to 6
- fwd_v: bfloat16 [8192, 4096], P('seq', 'chan'), may hold values from -6 to 6
- bwd_q: bfloat16 [8192, 4096], P('seq', 'chan'), may hold values from -6 to 6
- bwd_k: bfloat16 [8192, 4096], P('seq', 'chan'), may hold values from -6 to 6
- bwd_v: bfloat16 [8192, 4096], P('seq', 'chan'), may hold values from -6 to 6
- bwd_grad: bfloat16 [8192, 4096], P('seq', 'chan'), may hold values from -6 to 6
- filters: float32 [8192, 1024], P('seq', 'chan'), may hold values from -0.0625 to 0.0625
- skip: float32 [4096], P('chan'), may hold values from -4 to 4
Outputs:
- output: bfloat16 [8192, 4096], P('seq', 'chan')
- grad_query: bfloat16 [8192, 4096], P('seq', 'chan')
- grad_key: bfloat16 [8192, 4096], P('seq', 'chan')
- grad_value: bfloat16 [8192, 4096], P('seq', 'chan')
- grad_filter: float32 [8192, 1024], P('seq', 'chan')
- grad_skip: float32 [4096], P('chan')
The draws below stay inside these ranges and needn't reach their ends.
All inputs are finite; a program needn't handle non-finite values.
Results may differ from the reference program's by a relative error of at most 0.0075.
Values may be sent and summed in bfloat16 or wider, within the bound.
A program may use at most 256 MiB of HBM per device.

```python
import math
import jax
import jax.numpy as jnp
from jax import lax

C = 4096
FILTERS = 1024
SEQ_LEN = 8192


def block_scale(key, shape, shards, smallest, top_value):
    gain, own = 1.0, jax.random.fold_in(key, 6)
    for position, shards_of in shards:
        draws = jnp.exp(jax.random.uniform(jax.random.fold_in(own, position), (shards_of,), jnp.float32, smallest / len(shards), top_value / len(shards)))
        gain = gain * jnp.repeat(draws, shape[position] // shards_of).reshape([-1 if axis == position else 1 for axis in range(len(shape))])
    return gain


def bell_draw(own_key, extent, scale, limit, shards=(), kind=jnp.bfloat16):
    drawn = jax.random.normal(own_key, extent, jnp.float32) * scale
    if len(shards) > 0:
        drawn = block_scale(own_key, extent, shards, -0.22, 0.18) * drawn
    return jnp.clip(drawn, min=-limit, max=limit).astype(kind)


def setup_inputs(seed: int = 0) -> dict:
    streams_of = jax.random.split(jax.random.key(seed), 10)
    fwd_q = bell_draw(streams_of[0], (SEQ_LEN, C), 1.0, 6.0, ((0, 64), (1, 4)))
    fwd_k = bell_draw(streams_of[1], (SEQ_LEN, C), 1.0, 6.0, ((0, 64), (1, 4)))
    fwd_v = bell_draw(streams_of[2], (SEQ_LEN, C), 1.0, 6.0, ((0, 64), (1, 4)))
    bwd_q = bell_draw(streams_of[3], (SEQ_LEN, C), 1.0, 6.0, ((0, 64), (1, 4)))
    bwd_k = bell_draw(streams_of[4], (SEQ_LEN, C), 1.0, 6.0, ((0, 64), (1, 4)))
    bwd_v = bell_draw(streams_of[5], (SEQ_LEN, C), 1.0, 6.0, ((0, 64), (1, 4)))
    bwd_grad = bell_draw(streams_of[6], (SEQ_LEN, C), 1.0, 6.0, ((0, 64), (1, 4)))
    filters = bell_draw(streams_of[7], (SEQ_LEN, FILTERS), SEQ_LEN ** -0.5, 0.0625, ((0, 64), (1, 4)), jnp.float32)
    skip = bell_draw(streams_of[8], (C,), 1.0, 4.0, ((0, 4),), jnp.float32)
    return {"fwd_q": fwd_q, "fwd_k": fwd_k, "fwd_v": fwd_v, "bwd_q": bwd_q, "bwd_k": bwd_k, "bwd_v": bwd_v, "bwd_grad": bwd_grad, "filters": filters, "skip": skip}


def spectrum(values):
    return jnp.fft.rfft(values, n=2 * values.shape[0], axis=0)

def signal(spec, seq_length):
    return jnp.fft.irfft(spec, n=2 * seq_length, axis=0)[:seq_length]

def rounded(values):
    return lax.optimization_barrier(values.astype(jnp.bfloat16)).astype(jnp.float32)

def reference(fwd_q, fwd_k, fwd_v, bwd_q, bwd_k, bwd_v, bwd_grad, filters, skip):
    seq_length, channels = fwd_q.shape
    filter_count = filters.shape[1]
    grad_scale = 1.0 / math.sqrt(seq_length)
    filter_spec = spectrum(filters.astype(jnp.float32))
    out_parts, query_parts, key_parts, value_parts, skip_parts = ([], [], [], [], [])
    filter_total = jnp.zeros((seq_length, filter_count), jnp.float32)
    for group_index in range(channels // filter_count):
        start_col = group_index * filter_count
        stop_col = start_col + filter_count

        def column_block(array):
            return array[:, start_col:stop_col].astype(jnp.float32)
        skip_gain = skip[start_col:stop_col].astype(jnp.float32)
        source = rounded(column_block(fwd_k) * column_block(fwd_v))
        mixed = signal(filter_spec * spectrum(source), seq_length) + skip_gain * source
        out_parts.append((column_block(fwd_q) * mixed).astype(jnp.bfloat16))
        second_source = rounded(column_block(bwd_k) * column_block(bwd_v))
        second_spec = spectrum(second_source)
        mixed_two = signal(filter_spec * second_spec, seq_length) + skip_gain * second_source
        query_parts.append((column_block(bwd_grad) * mixed_two).astype(jnp.bfloat16))
        upstream = rounded(column_block(bwd_grad) * column_block(bwd_q))
        upstream_spec = spectrum(upstream)
        through = signal(jnp.conj(filter_spec) * upstream_spec, seq_length) + skip_gain * upstream
        key_parts.append((through * column_block(bwd_v)).astype(jnp.bfloat16))
        value_parts.append((through * column_block(bwd_k)).astype(jnp.bfloat16))
        filter_total = filter_total + signal(jnp.conj(second_spec) * upstream_spec, seq_length) * grad_scale
        skip_parts.append(lax.optimization_barrier(jnp.sum(upstream * second_source, axis=0)) * grad_scale)
    return (jnp.concatenate(out_parts, axis=1), jnp.concatenate(query_parts, axis=1), jnp.concatenate(key_parts, axis=1), jnp.concatenate(value_parts, axis=1), filter_total, jnp.concatenate(skip_parts, axis=0))
```

```python
import functools
import math

import jax
import jax.numpy as jnp
import numpy as np
from jax import lax
from jax.experimental import pallas as pl
from jax.experimental.pallas import tpu as pltpu
from jax.sharding import PartitionSpec as P

MESH = pl.DeviceIdType.MESH
F32 = jnp.float32
BF16 = jnp.bfloat16
ROWS = 128
SEQ = 64
HELD = 16
GROUPS = 4
PART = HELD // GROUPS
TOTAL = ROWS * SEQ
WIDTH = SEQ * HELD
QUARTER = SEQ * PART
SIGNALS = 4
DATA_LOW = True
TABLE_LOW = True


def halves(table):
    high = np.asarray(table, np.float32).astype(BF16)
    low = (np.asarray(table, np.float64) - high.astype(np.float64)).astype(np.float32).astype(BF16)
    return high, low


@functools.cache
def tables():
    row = np.arange(SEQ)
    lane = np.arange(ROWS)
    coarse = 2 * np.pi * ((row[None, :] * (4 * row[:, None] + 1)) % (4 * SEQ)) / (4 * SEQ)
    lead = np.concatenate([np.cos(coarse), -np.sin(coarse)], axis=0)
    lead = np.concatenate(halves(lead), axis=1)
    trail = np.concatenate([np.cos(coarse.T), -np.sin(coarse.T)], axis=1) / TOTAL
    trail = np.concatenate(halves(trail), axis=1)
    mid = 2 * np.pi * lane[None, :] * (4 * row[:, None] + 1) / (4 * TOTAL)
    twist = np.stack([np.cos(mid), np.sin(mid)]).astype(np.float32)
    fine = 2 * np.pi * ((lane[:, None] * lane[None, :]) % ROWS) / ROWS
    cosine, sine = np.cos(fine), np.sin(fine)
    ahead = np.stack(halves(np.block([[cosine, -sine], [sine, cosine]])))
    back = np.stack(halves(np.block([[cosine, sine], [-sine, cosine]])))
    return lead, trail, twist, ahead, back


def pack_kernel(fk, fv, bk, bv, bg, bq, fl, send, send_f, xs, fs):
    for m, (left, right) in enumerate(((fk, fv), (bk, bv), (bg, bq))):
        for b in range(WIDTH // ROWS):
            cols = slice(b * ROWS, (b + 1) * ROWS)
            xs[m, cols, :] = (left[:, cols].astype(F32) * right[:, cols].astype(F32)).T
    for b in range(QUARTER // ROWS):
        cols = slice(b * ROWS, (b + 1) * ROWS)
        fs[cols, :] = fl[:, cols].T

    def per_peer(step, carry):
        for k in range(8):
            peer = step * 8 + k
            for m in range(3):
                send[peer, m] = xs[m, pl.ds(peer, HELD, stride=SEQ), :].astype(BF16)
            send_f[peer] = fs[pl.ds(peer, PART, stride=SEQ), :].astype(BF16)
        return carry

    lax.fori_loop(0, SEQ // 8, per_peer, 0)


def pack(fk, fv, bk, bv, bg, bq, fl):
    return pl.pallas_call(
        pack_kernel,
        out_shape=(
            jax.ShapeDtypeStruct((SEQ, 3, HELD, ROWS), BF16),
            jax.ShapeDtypeStruct((SEQ, PART, ROWS), BF16),
        ),
        in_specs=[pl.BlockSpec(memory_space=pltpu.VMEM)] * 7,
        out_specs=[pl.BlockSpec(memory_space=pltpu.VMEM)] * 2,
        scratch_shapes=[pltpu.VMEM((3, WIDTH, ROWS), F32), pltpu.VMEM((QUARTER, ROWS), F32)],
    )(fk, fv, bk, bv, bg, bq, fl)


def dot(left, right):
    return jnp.dot(left, right, preferred_element_type=F32)


def split_dot(values, table):
    high = values.astype(BF16)
    total = dot(high, table[0])
    if DATA_LOW:
        total += dot((values - high.astype(F32)).astype(BF16), table[0])
    if TABLE_LOW:
        total += dot(high, table[1])
    return total


def times(a, b):
    return a[0] * b[0] - a[1] * b[1], a[0] * b[1] + a[1] * b[0]


def conj_times(a, b):
    return a[0] * b[0] + a[1] * b[1], a[0] * b[1] - a[1] * b[0]


def convolve_kernel(rx, filt, lead, trail, twist, ahead, back, y, terms, gs, xs, fs, ys, ts):
    def widen(step, carry):
        for k in range(8):
            s = step * 8 + k
            for m in range(3):
                xs[m, pl.ds(pl.multiple_of(s * HELD, HELD), HELD), :] = rx[s, m].astype(F32)
            for q in range(GROUPS):
                fs[q, pl.ds(s * PART, PART), :] = filt[q, s].astype(F32)
        return carry

    lax.fori_loop(0, SEQ // 8, widen, 0)
    gs[...] = jnp.zeros_like(gs)
    lane = lax.broadcasted_iota(jnp.int32, (1, ROWS), 1)

    def quarter(q, carry):
        chans = [(q * PART + r, r) for r in range(PART)]
        fronts = []
        for j, r in chans:
            cols = [xs[m, pl.ds(j, SEQ, stride=HELD), :] for m in range(3)]
            cols.append(fs[q, pl.ds(r, SEQ, stride=PART), :])
            total = jnp.sum(jnp.sum(cols[1] * cols[2], axis=0, keepdims=True), axis=1, keepdims=True)
            gs[...] += jnp.where(lane == j, total, 0.0)
            x = jnp.concatenate(cols, axis=1).astype(BF16)
            fronts.append(dot(lead[...], jnp.concatenate([x, x], axis=0)))
        spectra = []
        for front in fronts:
            rows = []
            for m in range(SIGNALS):
                real = front[:SEQ, m * ROWS : (m + 1) * ROWS]
                imag = front[SEQ:, m * ROWS : (m + 1) * ROWS]
                rows.append(
                    jnp.concatenate(
                        [real * twist[0] + imag * twist[1], imag * twist[0] - real * twist[1]], axis=1
                    )
                )
            spectra.append(split_dot(jnp.concatenate(rows, axis=0), ahead))
        products = []
        for spec in spectra:
            first, second, up, filt_spec = (
                (spec[m * SEQ : (m + 1) * SEQ, :ROWS], spec[m * SEQ : (m + 1) * SEQ, ROWS:])
                for m in range(SIGNALS)
            )
            made = (
                times(filt_spec, first),
                times(filt_spec, second),
                conj_times(filt_spec, up),
                conj_times(second, up),
            )
            rows = jnp.concatenate([jnp.concatenate(pair, axis=1) for pair in made], axis=0)
            products.append(split_dot(rows, back))
        for (j, r), rows in zip(chans, products):
            reals, imags = [], []
            for m in range(SIGNALS):
                real = rows[m * SEQ : (m + 1) * SEQ, :ROWS]
                imag = rows[m * SEQ : (m + 1) * SEQ, ROWS:]
                reals.append(real * twist[0] - imag * twist[1])
                imags.append(real * twist[1] + imag * twist[0])
            z = jnp.concatenate(
                [jnp.concatenate(reals, axis=1), jnp.concatenate(imags, axis=1)], axis=0
            )
            high = z.astype(BF16)
            final = dot(trail[...], jnp.concatenate([high, high], axis=0))
            if DATA_LOW:
                final += dot(trail[:, : 2 * SEQ], (z - high.astype(F32)).astype(BF16))
            for m in range(3):
                ys[m, pl.ds(j, SEQ, stride=HELD), :] = final[:, m * ROWS : (m + 1) * ROWS]
            ts[q, pl.ds(r, SEQ, stride=PART), :] = final[:, 3 * ROWS :]
        return carry

    lax.fori_loop(0, GROUPS, quarter, 0)
    gs[...] *= 1.0 / math.sqrt(TOTAL)

    def narrow(step, carry):
        for k in range(8):
            s = step * 8 + k
            for m in range(3):
                y[s, m] = ys[m, pl.ds(pl.multiple_of(s * HELD, HELD), HELD), :].astype(BF16)
        return carry

    lax.fori_loop(0, SEQ // 8, narrow, 0)
    for q in range(GROUPS):
        terms[q] = (ts[q] * (1.0 / math.sqrt(TOTAL))).astype(BF16)


def convolve(rx, filt):
    consts = [jnp.asarray(t) for t in tables()]
    return pl.pallas_call(
        convolve_kernel,
        out_shape=(
            jax.ShapeDtypeStruct((SEQ, 3, HELD, ROWS), BF16),
            jax.ShapeDtypeStruct((GROUPS, QUARTER, ROWS), BF16),
            jax.ShapeDtypeStruct((1, ROWS), F32),
        ),
        in_specs=[pl.BlockSpec(memory_space=pltpu.VMEM)] * 7,
        out_specs=[pl.BlockSpec(memory_space=pltpu.VMEM)] * 3,
        scratch_shapes=[
            pltpu.VMEM((3, WIDTH, ROWS), F32),
            pltpu.VMEM((GROUPS, QUARTER, ROWS), F32),
            pltpu.VMEM((3, WIDTH, ROWS), F32),
            pltpu.VMEM((GROUPS, QUARTER, ROWS), F32),
        ],
    )(rx, filt, *consts)


def finish_kernel(
    r, rf, rs, fq, fk, fv, bq, bk, bv, bg, skip, out, gq, gk, gv, gf, gsk, xs, fs, ss
):
    ss[...] = jnp.zeros_like(ss)

    def per_peer(step, carry):
        for k in range(8):
            peer = step * 8 + k
            for m in range(3):
                xs[m, pl.ds(peer, HELD, stride=SEQ), :] = r[peer, m].astype(F32)
            fs[pl.ds(peer, PART, stride=SEQ), :] = rf[peer].astype(F32)
            ss[pl.ds(peer, 1), :] = rs[peer]
        return carry

    lax.fori_loop(0, SEQ // 8, per_peer, 0)
    for b in range(WIDTH // ROWS):
        cols = slice(b * ROWS, (b + 1) * ROWS)
        gain = skip[:, cols]
        key, value = bk[:, cols].astype(F32), bv[:, cols].astype(F32)
        grad = bg[:, cols].astype(F32)
        source = (fk[:, cols].astype(F32) * fv[:, cols].astype(F32)).astype(BF16).astype(F32)
        second = (key * value).astype(BF16).astype(F32)
        upstream = (grad * bq[:, cols].astype(F32)).astype(BF16).astype(F32)
        out[:, cols] = (fq[:, cols].astype(F32) * (xs[0, cols, :].T + gain * source)).astype(BF16)
        gq[:, cols] = (grad * (xs[1, cols, :].T + gain * second)).astype(BF16)
        through = xs[2, cols, :].T + gain * upstream
        gk[:, cols] = (through * value).astype(BF16)
        gv[:, cols] = (through * key).astype(BF16)
    for b in range(QUARTER // ROWS):
        cols = slice(b * ROWS, (b + 1) * ROWS)
        gf[:, cols] = fs[cols, :].T
    ss[...] = ss[...].T
    even, odd = ss[pl.ds(0, 8, stride=2), :], ss[pl.ds(1, 8, stride=2), :]
    lane = lax.broadcasted_iota(jnp.int32, (8, ROWS), 1)
    gsk[...] = jnp.where(lane < SEQ, even, pltpu.roll(odd, SEQ, 1))


def finish(r, rf, rs, fq, fk, fv, bq, bk, bv, bg, skip):
    wide = jax.ShapeDtypeStruct((ROWS, WIDTH), BF16)
    return pl.pallas_call(
        finish_kernel,
        out_shape=(
            wide,
            wide,
            wide,
            wide,
            jax.ShapeDtypeStruct((ROWS, QUARTER), F32),
            jax.ShapeDtypeStruct((8, ROWS), F32),
        ),
        in_specs=[pl.BlockSpec(memory_space=pltpu.VMEM)] * 11,
        out_specs=[pl.BlockSpec(memory_space=pltpu.VMEM)] * 6,
        scratch_shapes=[
            pltpu.VMEM((3, WIDTH, ROWS), F32),
            pltpu.VMEM((QUARTER, ROWS), F32),
            pltpu.VMEM((ROWS, ROWS), F32),
        ],
    )(r, rf, rs, fq, fk, fv, bq, bk, bv, bg, skip)


def shifted(me, step):
    dz, dy, dx = step // 16, (step // 4) % 4, step % 4
    x, z, y = me // 16, (me // 4) % 4, me % 4
    return ((x + dx) % 4) * 16 + ((z + dz) % 4) * 4 + (y + dy) % 4


def greet(me, partners):
    barrier = pltpu.get_barrier_semaphore()

    def hello(step, carry):
        pl.semaphore_signal(
            barrier, inc=1, device_id={"seq": shifted(me, step)}, device_id_type=MESH
        )
        return carry

    lax.fori_loop(1, SEQ, hello, 0)
    for other in partners:
        pl.semaphore_signal(barrier, inc=1, device_id={"chan": other}, device_id_type=MESH)
    pl.semaphore_wait(barrier, SEQ - 1 + len(partners))


def push(src, dst, sems, target):
    copy = pltpu.make_async_remote_copy(
        src_ref=src,
        dst_ref=dst,
        send_sem=sems[0],
        recv_sem=sems[1],
        device_id=target,
        device_id_type=MESH,
    )
    copy.start()
    return copy


def push_all(src, dst, sems, me, first, last):
    def one(step, carry):
        peer = shifted(me, step)
        push(src.at[peer], dst.at[me], sems, {"seq": peer})
        return carry

    lax.fori_loop(first, last, one, 0)


def all_of(ref, sems, me):
    most = ref.at[pl.ds(0, SEQ - 1)]
    return pltpu.make_async_remote_copy(
        src_ref=most,
        dst_ref=most,
        send_sem=sems[0],
        recv_sem=sems[1],
        device_id={"seq": shifted(me, 1)},
        device_id_type=MESH,
    )


def partners_of(group):
    core, half = group % 2, group // 2
    return 2 * half + (1 - core), 2 * (1 - half) + core, 2 * (1 - half) + (1 - core)


def gather_kernel(send, send_f, recv, filt, s0, r0, s1, r1, s2, r2):
    me, group = lax.axis_index("seq"), lax.axis_index("chan")
    beside, across, corner = partners_of(group)
    greet(me, (beside, across))
    mine = filt.at[group]
    push_all(send_f, mine, (s1, r1), me, 1, SEQ)
    push_all(send, recv, (s0, r0), me, 1, 16)
    recv[me] = send[me]
    filt[group, me] = send_f[me]
    both = all_of(mine, (s1, r1), me)
    both.wait_recv()
    far = push(mine, mine, (s2.at[1], r2.at[1]), {"chan": across})
    near = push(mine, mine, (s2.at[0], r2.at[0]), {"chan": beside})
    push_all(send, recv, (s0, r0), me, 16, SEQ)
    far.wait_recv()
    other = filt.at[across]
    onward = push(other, other, (s2.at[2], r2.at[2]), {"chan": beside})
    near.wait_recv()
    onward.wait_recv()
    main = all_of(recv, (s0, r0), me)
    main.wait_recv()
    both.wait_send()
    far.wait_send()
    near.wait_send()
    onward.wait_send()
    main.wait_send()


def gather(send, send_f):
    return pl.pallas_call(
        gather_kernel,
        out_shape=(
            jax.ShapeDtypeStruct(send.shape, send.dtype),
            jax.ShapeDtypeStruct((GROUPS, *send_f.shape), send_f.dtype),
        ),
        in_specs=[pl.BlockSpec(memory_space=pltpu.VMEM)] * 2,
        out_specs=[pl.BlockSpec(memory_space=pltpu.VMEM)] * 2,
        scratch_shapes=[pltpu.SemaphoreType.DMA] * 4 + [pltpu.SemaphoreType.DMA((3,))] * 2,
        compiler_params=pltpu.CompilerParams(collective_id=0, has_side_effects=True),
    )(send, send_f)


def scatter_kernel(
    y, terms, gs, recv, recv_f, recv_s, near_in, far_in, far_out, total, send_f,
    s0, r0, s1, r1, s2, r2, s3, r3,
):
    me, group = lax.axis_index("seq"), lax.axis_index("chan")
    core, half = group % 2, group // 2
    beside, across, corner = partners_of(group)
    greet(me, (beside, across))
    pushed = [
        push(terms.at[2 * h + (1 - core)], near_in.at[h], (s2.at[h], r2.at[h]), {"chan": beside})
        for h in range(2)
    ]

    def skips(step, carry):
        peer = shifted(me, step)
        push(gs, recv_s.at[me], (s3, r3), {"seq": peer})
        return carry

    lax.fori_loop(1, SEQ, skips, 0)
    push_all(y, recv, (s0, r0), me, 1, 16)
    for copy in pushed:
        copy.wait_recv()
    away = 1 - half
    far_out[...] = (terms[2 * away + core].astype(F32) + near_in[away].astype(F32)).astype(BF16)
    far = push(far_out, far_in, (s2.at[2], r2.at[2]), {"chan": across})
    push_all(y, recv, (s0, r0), me, 16, SEQ)
    recv[me] = y[me]
    recv_s[me] = gs[...]
    total[...] = terms[group].astype(F32) + near_in[half].astype(F32)
    far.wait_recv()
    total[...] += far_in[...].astype(F32)

    def cut(step, carry):
        for k in range(8):
            s = step * 8 + k
            send_f[s] = total[pl.ds(s * PART, PART), :].astype(BF16)
        return carry

    lax.fori_loop(0, SEQ // 8, cut, 0)
    push_all(send_f, recv_f, (s1, r1), me, 1, SEQ)
    recv_f[me] = send_f[me]
    last = [all_of(recv, (s0, r0), me), all_of(recv_f, (s1, r1), me), all_of(recv_s, (s3, r3), me)]
    for copy in last:
        copy.wait_recv()
    for copy in last + pushed + [far]:
        copy.wait_send()


def scatter(y, terms, gs):
    return pl.pallas_call(
        scatter_kernel,
        out_shape=(
            jax.ShapeDtypeStruct(y.shape, y.dtype),
            jax.ShapeDtypeStruct((SEQ, PART, ROWS), BF16),
            jax.ShapeDtypeStruct((SEQ, 1, ROWS), F32),
        ),
        in_specs=[pl.BlockSpec(memory_space=pltpu.VMEM)] * 3,
        out_specs=[pl.BlockSpec(memory_space=pltpu.VMEM)] * 3,
        scratch_shapes=[
            pltpu.VMEM((2, QUARTER, ROWS), BF16),
            pltpu.VMEM((QUARTER, ROWS), BF16),
            pltpu.VMEM((QUARTER, ROWS), BF16),
            pltpu.VMEM((QUARTER, ROWS), F32),
            pltpu.VMEM((SEQ, PART, ROWS), BF16),
        ]
        + [pltpu.SemaphoreType.DMA] * 4
        + [pltpu.SemaphoreType.DMA((3,))] * 2
        + [pltpu.SemaphoreType.DMA] * 2,
        compiler_params=pltpu.CompilerParams(collective_id=1, has_side_effects=True),
    )(y, terms, gs)


def per_device(fwd_q, fwd_k, fwd_v, bwd_q, bwd_k, bwd_v, bwd_grad, filters, skip):
    send, send_f = pack(fwd_k, fwd_v, bwd_k, bwd_v, bwd_grad, bwd_q, filters)
    recv, filt = gather(send, send_f)
    y, terms, gs = convolve(recv, filt)
    back, back_f, back_s = scatter(y, terms, gs)
    *wide, skips = finish(
        back, back_f, back_s, fwd_q, fwd_k, fwd_v, bwd_q, bwd_k, bwd_v, bwd_grad, skip[None, :]
    )
    return (*wide, skips.reshape(WIDTH))


def solution(mesh):
    both = P("seq", "chan")
    return jax.shard_map(
        per_device,
        mesh=mesh,
        in_specs=(both,) * 8 + (P("chan"),),
        out_specs=(both,) * 5 + (P("chan"),),
        check_vma=False,
    )
```

```python
import functools
import math

import jax
import jax.numpy as jnp
import numpy as np
from jax import lax
from jax.experimental import pallas as pl
from jax.experimental.pallas import tpu as pltpu
from jax.sharding import PartitionSpec as P

MESH = pl.DeviceIdType.MESH
F32 = jnp.float32
BF16 = jnp.bfloat16
ROWS = 128
SEQ = 64
HELD = 16
GROUPS = 4
PART = HELD // GROUPS
TOTAL = ROWS * SEQ
WIDTH = SEQ * HELD
QUARTER = SEQ * PART
SIGNALS = 4
DATA_LOW = True
TABLE_LOW = True


def halves(table):
    high = np.asarray(table, np.float32).astype(BF16)
    low = (np.asarray(table, np.float64) - high.astype(np.float64)).astype(np.float32).astype(BF16)
    return high, low


@functools.cache
def tables():
    row = np.arange(SEQ)
    lane = np.arange(ROWS)
    coarse = 2 * np.pi * ((row[None, :] * (4 * row[:, None] + 1)) % (4 * SEQ)) / (4 * SEQ)
    lead = np.concatenate([np.cos(coarse), -np.sin(coarse)], axis=0)
    lead = np.concatenate(halves(lead), axis=1)
    trail = np.concatenate([np.cos(coarse.T), -np.sin(coarse.T)], axis=1) / TOTAL
    trail = np.concatenate(halves(trail), axis=1)
    mid = 2 * np.pi * lane[None, :] * (4 * row[:, None] + 1) / (4 * TOTAL)
    twist = np.stack([np.cos(mid), np.sin(mid)]).astype(np.float32)
    fine = 2 * np.pi * ((lane[:, None] * lane[None, :]) % ROWS) / ROWS
    cosine, sine = np.cos(fine), np.sin(fine)
    ahead = np.stack(halves(np.block([[cosine, -sine], [sine, cosine]])))
    back = np.stack(halves(np.block([[cosine, sine], [-sine, cosine]])))
    return lead, trail, twist, ahead, back


def dot(left, right):
    return jnp.dot(left, right, preferred_element_type=F32)


def split_dot(values, table):
    high = values.astype(BF16)
    total = dot(high, table[0])
    if DATA_LOW:
        total += dot((values - high.astype(F32)).astype(BF16), table[0])
    if TABLE_LOW:
        total += dot(high, table[1])
    return total


def times(a, b):
    return a[0] * b[0] - a[1] * b[1], a[0] * b[1] + a[1] * b[0]


def conj_times(a, b):
    return a[0] * b[0] + a[1] * b[1], a[0] * b[1] - a[1] * b[0]


def forward(cols, lead, twist, ahead):
    x = jnp.concatenate(cols, axis=1).astype(BF16)
    front = dot(lead[...], jnp.concatenate([x, x], axis=0))
    rows = []
    for m in range(len(cols)):
        real, imag = front[:SEQ, m * ROWS : (m + 1) * ROWS], front[SEQ:, m * ROWS : (m + 1) * ROWS]
        turned = [real * twist[0] + imag * twist[1], imag * twist[0] - real * twist[1]]
        rows.append(jnp.concatenate(turned, axis=1))
    spec = split_dot(jnp.concatenate(rows, axis=0), ahead)
    return [spec[m * SEQ : (m + 1) * SEQ] for m in range(len(cols))]


def inverse(pairs, trail, twist, back):
    rows = jnp.concatenate([jnp.concatenate(pair, axis=1) for pair in pairs], axis=0)
    rows = split_dot(rows, back)
    reals, imags = [], []
    for m in range(len(pairs)):
        real, imag = rows[m * SEQ : (m + 1) * SEQ, :ROWS], rows[m * SEQ : (m + 1) * SEQ, ROWS:]
        reals.append(real * twist[0] - imag * twist[1])
        imags.append(real * twist[1] + imag * twist[0])
    z = jnp.concatenate([jnp.concatenate(reals, axis=1), jnp.concatenate(imags, axis=1)], axis=0)
    high = z.astype(BF16)
    final = dot(trail[...], jnp.concatenate([high, high], axis=0))
    if DATA_LOW:
        final += dot(trail[:, : 2 * SEQ], (z - high.astype(F32)).astype(BF16))
    return [final[:, m * ROWS : (m + 1) * ROWS] for m in range(len(pairs))]


def pair_of(spec):
    return spec[:, :ROWS], spec[:, ROWS:]


def rows_of(s, count):
    return pl.ds(pl.multiple_of(s * count, count), count)


def in_steps(body):
    def step(n, carry):
        for k in range(8):
            body(n * 8 + k)
        return carry

    lax.fori_loop(0, SEQ // 8, step, 0)


def every_peer(me, body, itself=False):
    x, z, y = me // 16, (me // 4) % 4, me % 4
    zs = [((z + d) % 4) * 4 for d in range(4)]
    ys = [(y + d) % 4 for d in range(4)]
    steps = [(dz, dy) for dz in (2, 1, 3, 0) for dy in range(4)]

    def plane(dx, carry):
        base = ((x + dx) % 4) * 16
        for dz, dy in steps:
            body(base + zs[dz] + ys[dy])
        return carry

    for dz, dy in steps:
        if itself or (dz, dy) != (0, 0):
            body(x * 16 + zs[dz] + ys[dy])
    lax.fori_loop(1, 4, plane, 0)


def push(src, dst, sems, target):
    copy = pltpu.make_async_remote_copy(
        src_ref=src,
        dst_ref=dst,
        send_sem=sems[0],
        recv_sem=sems[1],
        device_id=target,
        device_id_type=MESH,
    )
    copy.start()
    return copy


def main_kernel(
    fk, fv, bk, bv, bg, bq, fl, lead, trail, twist, ahead, back,
    r, rf, rs,
    send, send_f, recv, filt, xs, fs, spectra, y, terms, near_in, out_f, gs, sent, got,
):
    me, group = lax.axis_index("seq"), lax.axis_index("chan")
    core, half = group % 2, group // 2
    beside, across = 2 * half + (1 - core), 2 * (1 - half) + core
    barrier = pltpu.get_barrier_semaphore()

    def hello(seq, chan):
        pl.semaphore_signal(
            barrier, inc=1, device_id={"seq": seq, "chan": chan}, device_id_type=MESH
        )

    every_peer(me, lambda peer: hello(peer, group))
    every_peer(me, lambda peer: hello(peer, across), True)
    hello(me, beside)

    def sems(n):
        return sent.at[n], got.at[n]

    def waiting(ref, n):
        return pltpu.make_async_remote_copy(
            src_ref=ref,
            dst_ref=ref,
            send_sem=sent.at[n],
            recv_sem=got.at[n],
            device_id={"chan": beside},
            device_id_type=MESH,
        )

    def most(ref):
        return ref.at[pl.ds(0, SEQ - 1)]

    def pack(m, left, right):
        for b in range(WIDTH // ROWS):
            cols = slice(b * ROWS, (b + 1) * ROWS)
            xs[m, cols, :] = (left[:, cols].astype(F32) * right[:, cols].astype(F32)).T

        def one(peer):
            send[m, peer] = xs[m, pl.ds(peer, HELD, stride=SEQ), :].astype(BF16)

        in_steps(one)

    def send_signal(m):
        every_peer(
            me, lambda peer: push(send.at[m, peer], recv.at[m, me], sems(m), {"seq": peer})
        )
        recv[m, me] = send[m, me]

    def widen(m):
        waiting(most(recv.at[m]), m).wait_recv()

        def one(s):
            xs[m, rows_of(s, HELD), :] = recv[m, s].astype(F32)

        in_steps(one)

    def send_back(m):
        def one(s):
            y[m, s] = xs[m, rows_of(s, HELD), :].astype(BF16)

        in_steps(one)
        every_peer(
            me, lambda peer: push(y.at[m, peer], r.at[m, me], sems(3 + m), {"seq": peer})
        )
        r[m, me] = y[m, me]

    for b in range(QUARTER // ROWS):
        cols = slice(b * ROWS, (b + 1) * ROWS)
        fs[0, cols, :] = fl[:, cols].T

    def filter_rows(peer):
        send_f[peer] = fs[0, pl.ds(peer, PART, stride=SEQ), :].astype(BF16)

    in_steps(filter_rows)
    pack(1, bk, bv)
    pl.semaphore_wait(barrier, 2 * SEQ)
    landing = filt.at[group, me]
    every_peer(me, lambda peer: push(send_f.at[peer], landing, sems(6), {"seq": peer}))
    every_peer(
        me,
        lambda peer: push(send_f.at[peer], landing, sems(7), {"seq": peer, "chan": across}),
        True,
    )
    filt[group, me] = send_f[me]
    send_signal(1)
    pack(2, bg, bq)
    send_signal(2)
    pack(0, fk, fv)
    send_signal(0)
    waiting(most(filt.at[group]), 6).wait_recv()
    waiting(filt.at[across], 7).wait_recv()
    moved = [
        push(filt.at[group], filt.at[group], sems(8), {"chan": beside}),
        push(filt.at[across], filt.at[across], sems(9), {"chan": beside}),
    ]
    for copy in moved:
        copy.wait_recv()

    def filter_wide(s):
        for q in range(GROUPS):
            fs[q, pl.ds(s * PART, PART), :] = filt[q, s].astype(F32)

    in_steps(filter_wide)

    def column(m, j):
        return xs[m, pl.ds(j, SEQ, stride=HELD), :]

    def store(m, j, value):
        xs[m, pl.ds(j, SEQ, stride=HELD), :] = value

    widen(1)

    def second(q, carry):
        cols = [column(1, q * PART + k) for k in range(PART)]
        cols += [fs[q, pl.ds(k, SEQ, stride=PART), :] for k in range(PART)]
        spec = forward(cols, lead, twist, ahead)
        pairs = []
        for k in range(PART):
            spectra[0, q * PART + k] = spec[k]
            spectra[1, q * PART + k] = spec[PART + k]
            pairs.append(times(pair_of(spec[PART + k]), pair_of(spec[k])))
        for k, value in enumerate(inverse(pairs, trail, twist, back)):
            store(3, q * PART + k, value)
        return carry

    lax.fori_loop(0, GROUPS, second, 0)

    def second_out(s):
        y[1, s] = xs[3, rows_of(s, HELD), :].astype(BF16)

    in_steps(second_out)
    every_peer(me, lambda peer: push(y.at[1, peer], r.at[1, me], sems(4), {"seq": peer}))
    r[1, me] = y[1, me]

    widen(2)
    gs[...] = jnp.zeros_like(gs)
    lane = lax.broadcasted_iota(jnp.int32, (1, ROWS), 1)
    scale = 1.0 / math.sqrt(TOTAL)

    def correlate(q, carry):
        cols = [column(2, q * PART + k) for k in range(PART)]
        for k in range(PART):
            part = jnp.sum(cols[k] * column(1, q * PART + k), axis=0, keepdims=True)
            part = jnp.sum(part, axis=1, keepdims=True)
            gs[...] += jnp.where(lane == q * PART + k, part * scale, 0.0)
        spec = forward(cols, lead, twist, ahead)
        pairs = []
        for k in range(PART):
            pairs.append(conj_times(pair_of(spectra[1, q * PART + k]), pair_of(spec[k])))
        for k in range(PART):
            pairs.append(conj_times(pair_of(spectra[0, q * PART + k]), pair_of(spec[k])))
        values = inverse(pairs, trail, twist, back)
        for k in range(PART):
            store(2, q * PART + k, values[k])
            fs[q, pl.ds(k, SEQ, stride=PART), :] = values[PART + k]
        return carry

    lax.fori_loop(0, GROUPS, correlate, 0)
    for q in range(GROUPS):
        terms[q] = (fs[q] * scale).astype(BF16)
    swapped = [
        push(terms.at[2 * h + (1 - core)], near_in.at[h], sems(10 + h), {"chan": beside})
        for h in range(2)
    ]
    send_back(2)
    for copy in swapped:
        copy.wait_recv()
    fs[0] = terms[group].astype(F32) + near_in[half].astype(F32)
    fs[1] = terms[across].astype(F32) + near_in[1 - half].astype(F32)

    def cut(s):
        for n in range(2):
            out_f[n, s] = fs[n, pl.ds(s * PART, PART), :].astype(BF16)

    in_steps(cut)

    def own_terms(peer):
        push(out_f.at[0, peer], rf.at[0, me], sems(12), {"seq": peer})
        push(gs, rs.at[me], sems(14), {"seq": peer})

    every_peer(me, own_terms)
    every_peer(
        me,
        lambda peer: push(
            out_f.at[1, peer], rf.at[1, me], sems(13), {"seq": peer, "chan": across}
        ),
        True,
    )
    rf[0, me] = out_f[0, me]
    rs[me] = gs[...]

    widen(0)

    def first(q, carry):
        cols = [column(0, q * PART + k) for k in range(PART)]
        spec = forward(cols, lead, twist, ahead)
        pairs = [
            times(pair_of(spectra[1, q * PART + k]), pair_of(spec[k])) for k in range(PART)
        ]
        for k, value in enumerate(inverse(pairs, trail, twist, back)):
            store(0, q * PART + k, value)
        return carry

    lax.fori_loop(0, GROUPS, first, 0)
    send_back(0)

    last = [waiting(most(r.at[m]), 3 + m) for m in range(3)]
    last += [waiting(most(rf.at[0]), 12), waiting(rf.at[1], 13), waiting(most(rs), 14)]
    for copy in last:
        copy.wait_recv()
    for m in range(3):
        waiting(most(send.at[m]), m).wait_send()
    waiting(most(send_f), 6).wait_send()
    waiting(send_f, 7).wait_send()
    for copy in moved + swapped + last:
        copy.wait_send()


def exchange(fk, fv, bk, bv, bg, bq, fl):
    consts = [jnp.asarray(t) for t in tables()]
    return pl.pallas_call(
        main_kernel,
        out_shape=(
            jax.ShapeDtypeStruct((3, SEQ, HELD, ROWS), BF16),
            jax.ShapeDtypeStruct((2, SEQ, PART, ROWS), BF16),
            jax.ShapeDtypeStruct((SEQ, 1, ROWS), F32),
        ),
        in_specs=[pl.BlockSpec(memory_space=pltpu.VMEM)] * 12,
        out_specs=[pl.BlockSpec(memory_space=pltpu.VMEM)] * 3,
        scratch_shapes=[
            pltpu.VMEM((3, SEQ, HELD, ROWS), BF16),
            pltpu.VMEM((SEQ, PART, ROWS), BF16),
            pltpu.VMEM((3, SEQ, HELD, ROWS), BF16),
            pltpu.VMEM((GROUPS, SEQ, PART, ROWS), BF16),
            pltpu.VMEM((4, WIDTH, ROWS), F32),
            pltpu.VMEM((GROUPS, QUARTER, ROWS), F32),
            pltpu.VMEM((2, HELD, SEQ, 2 * ROWS), F32),
            pltpu.VMEM((3, SEQ, HELD, ROWS), BF16),
            pltpu.VMEM((GROUPS, QUARTER, ROWS), BF16),
            pltpu.VMEM((2, QUARTER, ROWS), BF16),
            pltpu.VMEM((2, SEQ, PART, ROWS), BF16),
            pltpu.VMEM((1, ROWS), F32),
            pltpu.SemaphoreType.DMA((15,)),
            pltpu.SemaphoreType.DMA((15,)),
        ],
        compiler_params=pltpu.CompilerParams(collective_id=0, has_side_effects=True),
    )(fk, fv, bk, bv, bg, bq, fl, *consts)


def finish_kernel(
    r, rf, rs, fq, fk, fv, bq, bk, bv, bg, skip, out, gq, gk, gv, gf, gsk, xs, fs, ss
):
    ss[...] = jnp.zeros_like(ss)

    def per_peer(step, carry):
        for k in range(8):
            peer = step * 8 + k
            for m in range(3):
                xs[m, pl.ds(peer, HELD, stride=SEQ), :] = r[m, peer].astype(F32)
            fs[pl.ds(peer, PART, stride=SEQ), :] = rf[0, peer].astype(F32) + rf[1, peer].astype(F32)
            ss[pl.ds(peer, 1), :] = rs[peer]
        return carry

    lax.fori_loop(0, SEQ // 8, per_peer, 0)
    for b in range(WIDTH // ROWS):
        cols = slice(b * ROWS, (b + 1) * ROWS)
        gain = skip[:, cols]
        key, value = bk[:, cols].astype(F32), bv[:, cols].astype(F32)
        grad = bg[:, cols].astype(F32)
        source = (fk[:, cols].astype(F32) * fv[:, cols].astype(F32)).astype(BF16).astype(F32)
        second = (key * value).astype(BF16).astype(F32)
        upstream = (grad * bq[:, cols].astype(F32)).astype(BF16).astype(F32)
        out[:, cols] = (fq[:, cols].astype(F32) * (xs[0, cols, :].T + gain * source)).astype(BF16)
        gq[:, cols] = (grad * (xs[1, cols, :].T + gain * second)).astype(BF16)
        through = xs[2, cols, :].T + gain * upstream
        gk[:, cols] = (through * value).astype(BF16)
        gv[:, cols] = (through * key).astype(BF16)
    for b in range(QUARTER // ROWS):
        cols = slice(b * ROWS, (b + 1) * ROWS)
        gf[:, cols] = fs[cols, :].T
    ss[...] = ss[...].T
    even, odd = ss[pl.ds(0, 8, stride=2), :], ss[pl.ds(1, 8, stride=2), :]
    lane = lax.broadcasted_iota(jnp.int32, (8, ROWS), 1)
    gsk[...] = jnp.where(lane < SEQ, even, pltpu.roll(odd, SEQ, 1))


def finish(r, rf, rs, fq, fk, fv, bq, bk, bv, bg, skip):
    wide = jax.ShapeDtypeStruct((ROWS, WIDTH), BF16)
    return pl.pallas_call(
        finish_kernel,
        out_shape=(
            wide,
            wide,
            wide,
            wide,
            jax.ShapeDtypeStruct((ROWS, QUARTER), F32),
            jax.ShapeDtypeStruct((8, ROWS), F32),
        ),
        in_specs=[pl.BlockSpec(memory_space=pltpu.VMEM)] * 11,
        out_specs=[pl.BlockSpec(memory_space=pltpu.VMEM)] * 6,
        scratch_shapes=[
            pltpu.VMEM((3, WIDTH, ROWS), F32),
            pltpu.VMEM((QUARTER, ROWS), F32),
            pltpu.VMEM((ROWS, ROWS), F32),
        ],
    )(r, rf, rs, fq, fk, fv, bq, bk, bv, bg, skip)


def per_device(fwd_q, fwd_k, fwd_v, bwd_q, bwd_k, bwd_v, bwd_grad, filters, skip):
    back, back_f, back_s = exchange(fwd_k, fwd_v, bwd_k, bwd_v, bwd_grad, bwd_q, filters)
    *wide, skips = finish(
        back, back_f, back_s, fwd_q, fwd_k, fwd_v, bwd_q, bwd_k, bwd_v, bwd_grad, skip[None, :]
    )
    return (*wide, skips.reshape(WIDTH))


def solution(mesh):
    both = P("seq", "chan")
    return jax.shard_map(
        per_device,
        mesh=mesh,
        in_specs=(both,) * 8 + (P("chan"),),
        out_specs=(both,) * 5 + (P("chan"),),
        check_vma=False,
    )
```

```python
import functools
import math

import jax
import jax.numpy as jnp
import numpy as np
from jax import lax
from jax.experimental import pallas as pl
from jax.experimental.pallas import tpu as pltpu
from jax.sharding import PartitionSpec as P

MESH = pl.DeviceIdType.MESH
F32 = jnp.float32
BF16 = jnp.bfloat16
ROWS = 128
SEQ = 64
HELD = 16
GROUPS = 4
PART = HELD // GROUPS
TOTAL = ROWS * SEQ
WIDTH = SEQ * HELD
QUARTER = SEQ * PART
COPIED = 14
DATA_LOW = True
TABLE_LOW = True


def halves(table):
    high = np.asarray(table, np.float32).astype(BF16)
    low = (np.asarray(table, np.float64) - high.astype(np.float64)).astype(np.float32).astype(BF16)
    return high, low


@functools.cache
def tables():
    row = np.arange(SEQ)
    lane = np.arange(ROWS)
    coarse = 2 * np.pi * ((row[None, :] * (4 * row[:, None] + 1)) % (4 * SEQ)) / (4 * SEQ)
    lead = np.concatenate([np.cos(coarse), -np.sin(coarse)], axis=0)
    lead = np.concatenate(halves(lead), axis=1)
    trail = np.concatenate([np.cos(coarse.T), -np.sin(coarse.T)], axis=1) / TOTAL
    trail = np.concatenate(halves(trail), axis=1)
    mid = 2 * np.pi * lane[None, :] * (4 * row[:, None] + 1) / (4 * TOTAL)
    twist = np.stack([np.cos(mid), np.sin(mid)]).astype(np.float32)
    fine = 2 * np.pi * ((lane[:, None] * lane[None, :]) % ROWS) / ROWS
    cosine, sine = np.cos(fine), np.sin(fine)
    ahead = np.stack(halves(np.block([[cosine, -sine], [sine, cosine]])))
    back = np.stack(halves(np.block([[cosine, sine], [-sine, cosine]])))
    return lead, trail, twist, ahead, back


def dot(left, right):
    return jnp.dot(left, right, preferred_element_type=F32)


def split_dot(values, table):
    high = values.astype(BF16)
    total = dot(high, table[0])
    if DATA_LOW:
        total += dot((values - high.astype(F32)).astype(BF16), table[0])
    if TABLE_LOW:
        total += dot(high, table[1])
    return total


def times(a, b):
    return a[0] * b[0] - a[1] * b[1], a[0] * b[1] + a[1] * b[0]


def conj_times(a, b):
    return a[0] * b[0] + a[1] * b[1], a[0] * b[1] - a[1] * b[0]


def forward(cols, lead, twist, ahead):
    x = jnp.concatenate(cols, axis=1).astype(BF16)
    front = dot(lead[...], jnp.concatenate([x, x], axis=0))
    rows = []
    for m in range(len(cols)):
        real, imag = front[:SEQ, m * ROWS : (m + 1) * ROWS], front[SEQ:, m * ROWS : (m + 1) * ROWS]
        turned = [real * twist[0] + imag * twist[1], imag * twist[0] - real * twist[1]]
        rows.append(jnp.concatenate(turned, axis=1))
    spec = split_dot(jnp.concatenate(rows, axis=0), ahead)
    return [spec[m * SEQ : (m + 1) * SEQ] for m in range(len(cols))]


def inverse(pairs, trail, twist, back):
    rows = jnp.concatenate([jnp.concatenate(pair, axis=1) for pair in pairs], axis=0)
    rows = split_dot(rows, back)
    reals, imags = [], []
    for m in range(len(pairs)):
        real, imag = rows[m * SEQ : (m + 1) * SEQ, :ROWS], rows[m * SEQ : (m + 1) * SEQ, ROWS:]
        reals.append(real * twist[0] - imag * twist[1])
        imags.append(real * twist[1] + imag * twist[0])
    z = jnp.concatenate([jnp.concatenate(reals, axis=1), jnp.concatenate(imags, axis=1)], axis=0)
    high = z.astype(BF16)
    final = dot(trail[...], jnp.concatenate([high, high], axis=0))
    if DATA_LOW:
        final += dot(trail[:, : 2 * SEQ], (z - high.astype(F32)).astype(BF16))
    return [final[:, m * ROWS : (m + 1) * ROWS] for m in range(len(pairs))]


def pair_of(spec):
    return spec[:, :ROWS], spec[:, ROWS:]


def rows_of(s, count):
    return pl.ds(pl.multiple_of(s * count, count), count)


def in_steps(body):
    def step(n, carry):
        for k in range(8):
            body(n * 8 + k)
        return carry

    lax.fori_loop(0, SEQ // 8, step, 0)


def every_peer(me, body, itself=False):
    x, z, y = me // 16, (me // 4) % 4, me % 4
    ys = [(y + d) % 4 for d in (2, 1, 3, 0)]
    for other in (3 - z, (z + 2) % 4, z + 1 - 2 * (z % 2)):

        def plane(dx, carry, other=other):
            for y_other in ys:
                body(((x + dx) % 4) * 16 + other * 4 + y_other)
            return carry

        lax.fori_loop(0, 4, plane, 0)

    def level(dx, carry):
        for y_other in ys:
            body(((x + dx) % 4) * 16 + z * 4 + y_other)
        return carry

    lax.fori_loop(1, 4, level, 0)
    for y_other in ys if itself else ys[:3]:
        body(x * 16 + z * 4 + y_other)


def push(src, dst, sems, target):
    copy = pltpu.make_async_remote_copy(
        src_ref=src,
        dst_ref=dst,
        send_sem=sems[0],
        recv_sem=sems[1],
        device_id=target,
        device_id_type=MESH,
    )
    copy.start()
    return copy


def main_kernel(*refs):
    sources, (out, gq, gk, gv, gf, gsk) = refs[:COPIED], refs[COPIED : COPIED + 6]
    copied, loaded = refs[COPIED + 6 : 2 * COPIED + 6], refs[2 * COPIED + 6]
    (
        r, rf, rs, send, send_f, recv, filt, xs, fs, ss, spectra, y, terms, near_in, out_f, gs,
        sent, got,
    ) = refs[2 * COPIED + 7 :]
    fl, bk, bv, bg, bq, fk, fv, lead, trail, twist, ahead, back, fq, skip = copied
    me, group = lax.axis_index("seq"), lax.axis_index("chan")
    core, half = group % 2, group // 2
    beside, across = 2 * half + (1 - core), 2 * (1 - half) + core
    barrier = pltpu.get_barrier_semaphore()
    loads = [
        pltpu.make_async_copy(sources[n], copied[n], loaded.at[n]) for n in range(COPIED)
    ]
    for load in loads:
        load.start()

    def hello(seq, chan):
        pl.semaphore_signal(
            barrier, inc=1, device_id={"seq": seq, "chan": chan}, device_id_type=MESH
        )

    every_peer(me, lambda peer: hello(peer, across), True)
    every_peer(me, lambda peer: hello(peer, group))
    hello(me, beside)

    def sems(n):
        return sent.at[n], got.at[n]

    def waiting(ref, n):
        return pltpu.make_async_remote_copy(
            src_ref=ref,
            dst_ref=ref,
            send_sem=sent.at[n],
            recv_sem=got.at[n],
            device_id={"chan": beside},
            device_id_type=MESH,
        )

    def most(ref):
        return ref.at[pl.ds(0, SEQ - 1)]

    def pack(m, left, right):
        for b in range(WIDTH // ROWS):
            cols = slice(b * ROWS, (b + 1) * ROWS)
            xs[m, cols, :] = (left[:, cols].astype(F32) * right[:, cols].astype(F32)).T

        def one(peer):
            send[m, peer] = xs[m, pl.ds(peer, HELD, stride=SEQ), :].astype(BF16)

        in_steps(one)

    def send_signal(m):
        every_peer(
            me, lambda peer: push(send.at[m, peer], recv.at[m, me], sems(m), {"seq": peer})
        )
        recv[m, me] = send[m, me]

    def widen(m):
        waiting(most(recv.at[m]), m).wait_recv()

        def one(s):
            xs[m, rows_of(s, HELD), :] = recv[m, s].astype(F32)

        in_steps(one)

    def send_back(m):
        def one(s):
            y[m, s] = xs[m, rows_of(s, HELD), :].astype(BF16)

        in_steps(one)
        every_peer(
            me, lambda peer: push(y.at[m, peer], r.at[m, me], sems(3 + m), {"seq": peer})
        )
        r[m, me] = y[m, me]

    loads[0].wait()
    for b in range(QUARTER // ROWS):
        cols = slice(b * ROWS, (b + 1) * ROWS)
        fs[0, cols, :] = fl[:, cols].T

    def filter_rows(peer):
        send_f[peer] = fs[0, pl.ds(peer, PART, stride=SEQ), :].astype(BF16)

    in_steps(filter_rows)
    loads[1].wait()
    loads[2].wait()
    pack(1, bk, bv)
    pl.semaphore_wait(barrier, 2 * SEQ)
    landing = filt.at[group, me]
    every_peer(me, lambda peer: push(send_f.at[peer], landing, sems(6), {"seq": peer}))
    every_peer(
        me,
        lambda peer: push(send_f.at[peer], landing, sems(7), {"seq": peer, "chan": across}),
        True,
    )
    filt[group, me] = send_f[me]
    send_signal(1)
    loads[3].wait()
    loads[4].wait()
    pack(2, bg, bq)
    send_signal(2)
    loads[5].wait()
    loads[6].wait()
    pack(0, fk, fv)
    send_signal(0)
    for load in loads[7:]:
        load.wait()
    waiting(most(filt.at[group]), 6).wait_recv()
    waiting(filt.at[across], 7).wait_recv()
    moved = [
        push(filt.at[group], filt.at[group], sems(8), {"chan": beside}),
        push(filt.at[across], filt.at[across], sems(9), {"chan": beside}),
    ]
    for copy in moved:
        copy.wait_recv()

    def filter_wide(s):
        for q in range(GROUPS):
            fs[q, pl.ds(s * PART, PART), :] = filt[q, s].astype(F32)

    in_steps(filter_wide)

    def column(m, j):
        return xs[m, pl.ds(j, SEQ, stride=HELD), :]

    def put(m, j, value):
        xs[m, pl.ds(j, SEQ, stride=HELD), :] = value

    widen(1)

    def second(q, carry):
        cols = [column(1, q * PART + k) for k in range(PART)]
        cols += [fs[q, pl.ds(k, SEQ, stride=PART), :] for k in range(PART)]
        spec = forward(cols, lead, twist, ahead)
        pairs = []
        for k in range(PART):
            spectra[0, q * PART + k] = spec[k]
            spectra[1, q * PART + k] = spec[PART + k]
            pairs.append(times(pair_of(spec[PART + k]), pair_of(spec[k])))
        for k, value in enumerate(inverse(pairs, trail, twist, back)):
            put(3, q * PART + k, value)
        return carry

    lax.fori_loop(0, GROUPS, second, 0)

    def second_out(s):
        y[1, s] = xs[3, rows_of(s, HELD), :].astype(BF16)

    in_steps(second_out)
    every_peer(me, lambda peer: push(y.at[1, peer], r.at[1, me], sems(4), {"seq": peer}))
    r[1, me] = y[1, me]

    widen(2)
    gs[...] = jnp.zeros_like(gs)
    lane = lax.broadcasted_iota(jnp.int32, (1, ROWS), 1)
    scale = 1.0 / math.sqrt(TOTAL)

    def correlate(q, carry):
        cols = [column(2, q * PART + k) for k in range(PART)]
        for k in range(PART):
            part = jnp.sum(cols[k] * column(1, q * PART + k), axis=0, keepdims=True)
            part = jnp.sum(part, axis=1, keepdims=True)
            gs[...] += jnp.where(lane == q * PART + k, part * scale, 0.0)
        spec = forward(cols, lead, twist, ahead)
        pairs = []
        for k in range(PART):
            pairs.append(conj_times(pair_of(spectra[1, q * PART + k]), pair_of(spec[k])))
        for k in range(PART):
            pairs.append(conj_times(pair_of(spectra[0, q * PART + k]), pair_of(spec[k])))
        values = inverse(pairs, trail, twist, back)
        for k in range(PART):
            put(2, q * PART + k, values[k])
            fs[q, pl.ds(k, SEQ, stride=PART), :] = values[PART + k]
        return carry

    lax.fori_loop(0, GROUPS, correlate, 0)
    for q in range(GROUPS):
        terms[q] = (fs[q] * scale).astype(BF16)
    swapped = [
        push(terms.at[2 * h + (1 - core)], near_in.at[h], sems(10 + h), {"chan": beside})
        for h in range(2)
    ]
    send_back(2)
    for copy in swapped:
        copy.wait_recv()
    fs[0] = terms[group].astype(F32) + near_in[half].astype(F32)
    fs[1] = terms[across].astype(F32) + near_in[1 - half].astype(F32)

    def cut(s):
        for n in range(2):
            out_f[n, s] = fs[n, pl.ds(s * PART, PART), :].astype(BF16)

    in_steps(cut)

    def own_terms(peer):
        push(out_f.at[0, peer], rf.at[0, me], sems(12), {"seq": peer})
        push(gs, rs.at[me], sems(14), {"seq": peer})

    every_peer(me, own_terms)
    every_peer(
        me,
        lambda peer: push(
            out_f.at[1, peer], rf.at[1, me], sems(13), {"seq": peer, "chan": across}
        ),
        True,
    )
    rf[0, me] = out_f[0, me]
    rs[me] = gs[...]

    widen(0)

    def first(q, carry):
        cols = [column(0, q * PART + k) for k in range(PART)]
        spec = forward(cols, lead, twist, ahead)
        pairs = [
            times(pair_of(spectra[1, q * PART + k]), pair_of(spec[k])) for k in range(PART)
        ]
        for k, value in enumerate(inverse(pairs, trail, twist, back)):
            put(0, q * PART + k, value)
        return carry

    lax.fori_loop(0, GROUPS, first, 0)
    send_back(0)

    def unpack(m):
        waiting(most(r.at[m]), 3 + m).wait_recv()

        def one(peer):
            xs[m, pl.ds(peer, HELD, stride=SEQ), :] = r[m, peer].astype(F32)

        in_steps(one)

    def product(left, right):
        return (left.astype(F32) * right.astype(F32)).astype(BF16).astype(F32)

    blocks = [slice(b * ROWS, (b + 1) * ROWS) for b in range(WIDTH // ROWS)]
    unpack(1)
    for cols in blocks:
        mixed = xs[1, cols, :].T + skip[:, cols] * product(bk[:, cols], bv[:, cols])
        gq[:, cols] = (bg[:, cols].astype(F32) * mixed).astype(BF16)
    unpack(2)
    for cols in blocks:
        through = xs[2, cols, :].T + skip[:, cols] * product(bg[:, cols], bq[:, cols])
        gk[:, cols] = (through * bv[:, cols].astype(F32)).astype(BF16)
        gv[:, cols] = (through * bk[:, cols].astype(F32)).astype(BF16)
    last = [waiting(most(rf.at[0]), 12), waiting(rf.at[1], 13), waiting(most(rs), 14)]
    for copy in last:
        copy.wait_recv()
    ss[...] = jnp.zeros_like(ss)

    def unpack_terms(peer):
        fs[0, pl.ds(peer, PART, stride=SEQ), :] = rf[0, peer].astype(F32) + rf[1, peer].astype(F32)
        ss[pl.ds(peer, 1), :] = rs[peer]

    in_steps(unpack_terms)
    for cols in blocks[: QUARTER // ROWS]:
        gf[:, cols] = fs[0, cols, :].T
    ss[...] = ss[...].T
    even, odd = ss[pl.ds(0, 8, stride=2), :], ss[pl.ds(1, 8, stride=2), :]
    wide = lax.broadcasted_iota(jnp.int32, (8, ROWS), 1)
    gsk[...] = jnp.where(wide < SEQ, even, pltpu.roll(odd, SEQ, 1))
    unpack(0)
    for cols in blocks:
        mixed = xs[0, cols, :].T + skip[:, cols] * product(fk[:, cols], fv[:, cols])
        out[:, cols] = (fq[:, cols].astype(F32) * mixed).astype(BF16)
    for m in range(3):
        waiting(most(send.at[m]), m).wait_send()
        waiting(most(r.at[m]), 3 + m).wait_send()
    waiting(most(send_f), 6).wait_send()
    waiting(send_f, 7).wait_send()
    for copy in moved + swapped + last:
        copy.wait_send()


def exchange(fl, bk, bv, bg, bq, fk, fv, fq, skip):
    values = (fl, bk, bv, bg, bq, fk, fv, *[jnp.asarray(t) for t in tables()], fq, skip)
    wide = pltpu.VMEM((ROWS, WIDTH), BF16)
    return pl.pallas_call(
        main_kernel,
        out_shape=(
            wide,
            wide,
            wide,
            wide,
            pltpu.VMEM((ROWS, QUARTER), F32),
            pltpu.VMEM((8, ROWS), F32),
        ),
        in_specs=[pl.BlockSpec(memory_space=pltpu.HBM)] * COPIED,
        out_specs=[pl.BlockSpec(memory_space=pltpu.VMEM)] * 6,
        scratch_shapes=[
            *[pltpu.VMEM(v.shape, v.dtype) for v in values],
            pltpu.SemaphoreType.DMA((COPIED,)),
            pltpu.VMEM((3, SEQ, HELD, ROWS), BF16),
            pltpu.VMEM((2, SEQ, PART, ROWS), BF16),
            pltpu.VMEM((SEQ, 1, ROWS), F32),
            pltpu.VMEM((3, SEQ, HELD, ROWS), BF16),
            pltpu.VMEM((SEQ, PART, ROWS), BF16),
            pltpu.VMEM((3, SEQ, HELD, ROWS), BF16),
            pltpu.VMEM((GROUPS, SEQ, PART, ROWS), BF16),
            pltpu.VMEM((4, WIDTH, ROWS), F32),
            pltpu.VMEM((GROUPS, QUARTER, ROWS), F32),
            pltpu.VMEM((ROWS, ROWS), F32),
            pltpu.VMEM((2, HELD, SEQ, 2 * ROWS), F32),
            pltpu.VMEM((3, SEQ, HELD, ROWS), BF16),
            pltpu.VMEM((GROUPS, QUARTER, ROWS), BF16),
            pltpu.VMEM((2, QUARTER, ROWS), BF16),
            pltpu.VMEM((2, SEQ, PART, ROWS), BF16),
            pltpu.VMEM((1, ROWS), F32),
            pltpu.SemaphoreType.DMA((15,)),
            pltpu.SemaphoreType.DMA((15,)),
        ],
        compiler_params=pltpu.CompilerParams(collective_id=0, has_side_effects=True),
    )(*values)


def store_kernel(*refs):
    count = len(refs) // 2
    sems = refs[-1]
    copies = [
        pltpu.make_async_copy(refs[n], refs[count + n], sems.at[n]) for n in range(count)
    ]
    for copy in copies:
        copy.start()
    for copy in copies:
        copy.wait()


def store(values):
    return pl.pallas_call(
        store_kernel,
        out_shape=tuple(jax.ShapeDtypeStruct(v.shape, v.dtype) for v in values),
        in_specs=[pl.BlockSpec(memory_space=pltpu.VMEM)] * len(values),
        out_specs=[pl.BlockSpec(memory_space=pl.ANY)] * len(values),
        scratch_shapes=[pltpu.SemaphoreType.DMA((len(values),))],
    )(*[pltpu.with_memory_space_constraint(v, pltpu.VMEM) for v in values])


def per_device(fwd_q, fwd_k, fwd_v, bwd_q, bwd_k, bwd_v, bwd_grad, filters, skip):
    done = exchange(
        filters, bwd_k, bwd_v, bwd_grad, bwd_q, fwd_k, fwd_v, fwd_q, skip[None, :]
    )
    *wide, skips = store(done)
    return (*wide, skips.reshape(WIDTH))


def solution(mesh):
    both = P("seq", "chan")
    return jax.shard_map(
        per_device,
        mesh=mesh,
        in_specs=(both,) * 8 + (P("chan"),),
        out_specs=(both,) * 5 + (P("chan"),),
        check_vma=False,
    )
```

```python
import functools
import math

import jax
import jax.numpy as jnp
import numpy as np
from jax import lax
from jax.experimental import pallas as pl
from jax.experimental.pallas import tpu as pltpu
from jax.sharding import PartitionSpec as P

MESH = pl.DeviceIdType.MESH
F32 = jnp.float32
BF16 = jnp.bfloat16
ROWS = 128
SEQ = 64
HELD = 16
GROUPS = 4
PART = HELD // GROUPS
TOTAL = ROWS * SEQ
WIDTH = SEQ * HELD
QUARTER = SEQ * PART
COPIED = 14
DATA_LOW = True
TABLE_LOW = True


def halves(table):
    high = np.asarray(table, np.float32).astype(BF16)
    low = (np.asarray(table, np.float64) - high.astype(np.float64)).astype(np.float32).astype(BF16)
    return high, low


@functools.cache
def tables():
    row = np.arange(SEQ)
    lane = np.arange(ROWS)
    coarse = 2 * np.pi * ((row[None, :] * (4 * row[:, None] + 1)) % (4 * SEQ)) / (4 * SEQ)
    lead = np.concatenate([np.cos(coarse), -np.sin(coarse)], axis=0)
    lead = np.concatenate(halves(lead), axis=1)
    trail = np.concatenate([np.cos(coarse.T), -np.sin(coarse.T)], axis=1) / TOTAL
    trail = np.concatenate(halves(trail), axis=1)
    mid = 2 * np.pi * lane[None, :] * (4 * row[:, None] + 1) / (4 * TOTAL)
    twist = np.stack([np.cos(mid), np.sin(mid)]).astype(np.float32)
    fine = 2 * np.pi * ((lane[:, None] * lane[None, :]) % ROWS) / ROWS
    cosine, sine = np.cos(fine), np.sin(fine)
    ahead = np.stack(halves(np.block([[cosine, -sine], [sine, cosine]])))
    back = np.stack(halves(np.block([[cosine, sine], [-sine, cosine]])))
    return lead, trail, twist, ahead, back


def dot(left, right):
    return jnp.dot(left, right, preferred_element_type=F32)


def split_dot(values, table):
    high = values.astype(BF16)
    total = dot(high, table[0])
    if DATA_LOW:
        total += dot((values - high.astype(F32)).astype(BF16), table[0])
    if TABLE_LOW:
        total += dot(high, table[1])
    return total


def times(a, b):
    return a[0] * b[0] - a[1] * b[1], a[0] * b[1] + a[1] * b[0]


def conj_times(a, b):
    return a[0] * b[0] + a[1] * b[1], a[0] * b[1] - a[1] * b[0]


def forward(cols, lead, twist, ahead):
    x = jnp.concatenate(cols, axis=1).astype(BF16)
    front = dot(lead[...], jnp.concatenate([x, x], axis=0))
    rows = []
    for m in range(len(cols)):
        real, imag = front[:SEQ, m * ROWS : (m + 1) * ROWS], front[SEQ:, m * ROWS : (m + 1) * ROWS]
        turned = [real * twist[0] + imag * twist[1], imag * twist[0] - real * twist[1]]
        rows.append(jnp.concatenate(turned, axis=1))
    spec = split_dot(jnp.concatenate(rows, axis=0), ahead)
    return [spec[m * SEQ : (m + 1) * SEQ] for m in range(len(cols))]


def inverse(pairs, trail, twist, back):
    rows = jnp.concatenate([jnp.concatenate(pair, axis=1) for pair in pairs], axis=0)
    rows = split_dot(rows, back)
    reals, imags = [], []
    for m in range(len(pairs)):
        real, imag = rows[m * SEQ : (m + 1) * SEQ, :ROWS], rows[m * SEQ : (m + 1) * SEQ, ROWS:]
        reals.append(real * twist[0] - imag * twist[1])
        imags.append(real * twist[1] + imag * twist[0])
    z = jnp.concatenate([jnp.concatenate(reals, axis=1), jnp.concatenate(imags, axis=1)], axis=0)
    high = z.astype(BF16)
    final = dot(trail[...], jnp.concatenate([high, high], axis=0))
    if DATA_LOW:
        final += dot(trail[:, : 2 * SEQ], (z - high.astype(F32)).astype(BF16))
    return [final[:, m * ROWS : (m + 1) * ROWS] for m in range(len(pairs))]


def pair_of(spec):
    return spec[:, :ROWS], spec[:, ROWS:]


def rows_of(s, count):
    return pl.ds(pl.multiple_of(s * count, count), count)


def in_steps(body):
    def step(n, carry):
        for k in range(8):
            body(n * 8 + k)
        return carry

    lax.fori_loop(0, SEQ // 8, step, 0)


def every_peer(me, body, itself=False):
    x, z, y = me // 16, (me // 4) % 4, me % 4
    ys = [(y + d) % 4 for d in (2, 1, 3, 0)]
    for other in (3 - z, (z + 2) % 4, z + 1 - 2 * (z % 2)):

        def plane(dx, carry, other=other):
            for y_other in ys:
                body(((x + dx) % 4) * 16 + other * 4 + y_other)
            return carry

        lax.fori_loop(0, 4, plane, 0)

    def level(dx, carry):
        for y_other in ys:
            body(((x + dx) % 4) * 16 + z * 4 + y_other)
        return carry

    lax.fori_loop(1, 4, level, 0)
    for y_other in ys if itself else ys[:3]:
        body(x * 16 + z * 4 + y_other)


def every_peer_flat(me, body, itself=False):
    x, z, y = me // 16, (me // 4) % 4, me % 4
    xs = [((x + d) % 4) * 16 for d in (2, 1, 3, 0)]
    ys = [(y + d) % 4 for d in (2, 1, 3, 0)]
    for n, other in enumerate((3 - z, (z + 2) % 4, z + 1 - 2 * (z % 2), z)):
        for a in range(4):
            for b in range(4):
                if itself or (n, a, b) != (3, 3, 3):
                    body(xs[a] + other * 4 + ys[b])


def push(src, dst, sems, target):
    copy = pltpu.make_async_remote_copy(
        src_ref=src,
        dst_ref=dst,
        send_sem=sems[0],
        recv_sem=sems[1],
        device_id=target,
        device_id_type=MESH,
    )
    copy.start()
    return copy


def main_kernel(*refs):
    sources, (out, gq, gk, gv, gf, gsk) = refs[:COPIED], refs[COPIED : COPIED + 6]
    copied, loaded = refs[COPIED + 6 : 2 * COPIED + 6], refs[2 * COPIED + 6]
    (
        r, rf, rs, send, send_f, recv, filt, xs, fs, ss, spectra, y, terms, near_in, out_f, gs,
        sent, got, ready,
    ) = refs[2 * COPIED + 7 :]
    fl, bk, bv, bg, bq, fk, fv, lead, trail, twist, ahead, back, fq, skip = copied
    me, group = lax.axis_index("seq"), lax.axis_index("chan")
    core, half = group % 2, group // 2
    beside, across = 2 * half + (1 - core), 2 * (1 - half) + core
    barrier = pltpu.get_barrier_semaphore()
    loads = [
        pltpu.make_async_copy(sources[n], copied[n], loaded.at[n]) for n in range(COPIED)
    ]
    for load in loads:
        load.start()

    def hello(seq, chan, sem=barrier):
        pl.semaphore_signal(
            sem, inc=1, device_id={"seq": seq, "chan": chan}, device_id_type=MESH
        )

    every_peer_flat(me, lambda peer: hello(peer, group))
    hello(me, beside)

    @pl.when(half == 0)
    def _():
        every_peer_flat(me, lambda peer: hello(peer, across), True)


    def sems(n):
        return sent.at[n], got.at[n]

    def waiting(ref, n):
        return pltpu.make_async_remote_copy(
            src_ref=ref,
            dst_ref=ref,
            send_sem=sent.at[n],
            recv_sem=got.at[n],
            device_id={"chan": beside},
            device_id_type=MESH,
        )

    def most(ref):
        return ref.at[pl.ds(0, SEQ - 1)]

    def pack(m, left, right):
        for b in range(WIDTH // ROWS):
            cols = slice(b * ROWS, (b + 1) * ROWS)
            xs[m, cols, :] = (left[:, cols].astype(F32) * right[:, cols].astype(F32)).T

        def one(peer):
            send[m, peer] = xs[m, pl.ds(peer, HELD, stride=SEQ), :].astype(BF16)

        in_steps(one)

    def send_signal(m):
        every_peer(
            me, lambda peer: push(send.at[m, peer], recv.at[m, me], sems(m), {"seq": peer})
        )
        recv[m, me] = send[m, me]

    def widen(m):
        waiting(most(recv.at[m]), m).wait_recv()

        def one(s):
            xs[m, rows_of(s, HELD), :] = recv[m, s].astype(F32)

        in_steps(one)

    def send_back(m):
        def one(s):
            y[m, s] = xs[m, rows_of(s, HELD), :].astype(BF16)

        in_steps(one)
        every_peer(
            me, lambda peer: push(y.at[m, peer], r.at[m, me], sems(3 + m), {"seq": peer})
        )
        r[m, me] = y[m, me]

    loads[0].wait()
    for b in range(QUARTER // ROWS):
        cols = slice(b * ROWS, (b + 1) * ROWS)
        fs[0, cols, :] = fl[:, cols].T

    def filter_rows(peer):
        send_f[peer] = fs[0, pl.ds(peer, PART, stride=SEQ), :].astype(BF16)

    in_steps(filter_rows)
    loads[1].wait()
    loads[2].wait()
    pack(1, bk, bv)
    pl.semaphore_wait(barrier, SEQ + SEQ * half)
    landing = filt.at[group, me]

    def filters_across():
        every_peer(
            me,
            lambda peer: push(send_f.at[peer], landing, sems(7), {"seq": peer, "chan": across}),
            True,
        )

    @pl.when(half == 1)
    def _():
        every_peer_flat(me, lambda peer: hello(peer, across, ready), True)
        filters_across()

    every_peer(me, lambda peer: push(send_f.at[peer], landing, sems(6), {"seq": peer}))
    filt[group, me] = send_f[me]
    send_signal(1)
    loads[3].wait()
    loads[4].wait()
    pack(2, bg, bq)

    @pl.when(half == 0)
    def _():
        pl.semaphore_wait(ready, SEQ)
        filters_across()

    send_signal(2)
    loads[5].wait()
    loads[6].wait()
    pack(0, fk, fv)
    send_signal(0)
    for load in loads[7:]:
        load.wait()
    moved = []
    for held, landed in ((most(filt.at[group]), 6), (filt.at[across], 7)):
        waiting(held, landed).wait_recv()
        whole = filt.at[group if landed == 6 else across]
        moved.append(push(whole, whole, sems(landed + 2), {"chan": beside}))
    for copy in moved:
        copy.wait_recv()

    def filter_wide(s):
        for q in range(GROUPS):
            fs[q, pl.ds(s * PART, PART), :] = filt[q, s].astype(F32)

    in_steps(filter_wide)

    def column(m, j):
        return xs[m, pl.ds(j, SEQ, stride=HELD), :]

    def put(m, j, value):
        xs[m, pl.ds(j, SEQ, stride=HELD), :] = value

    widen(1)

    def second(q, carry):
        cols = [column(1, q * PART + k) for k in range(PART)]
        cols += [fs[q, pl.ds(k, SEQ, stride=PART), :] for k in range(PART)]
        spec = forward(cols, lead, twist, ahead)
        pairs = []
        for k in range(PART):
            spectra[0, q * PART + k] = spec[k]
            spectra[1, q * PART + k] = spec[PART + k]
            pairs.append(times(pair_of(spec[PART + k]), pair_of(spec[k])))
        for k, value in enumerate(inverse(pairs, trail, twist, back)):
            put(3, q * PART + k, value)
        return carry

    lax.fori_loop(0, GROUPS, second, 0)

    def second_out(s):
        y[1, s] = xs[3, rows_of(s, HELD), :].astype(BF16)

    in_steps(second_out)
    every_peer(me, lambda peer: push(y.at[1, peer], r.at[1, me], sems(4), {"seq": peer}))
    r[1, me] = y[1, me]

    widen(2)
    gs[...] = jnp.zeros_like(gs)
    lane = lax.broadcasted_iota(jnp.int32, (1, ROWS), 1)
    scale = 1.0 / math.sqrt(TOTAL)

    def correlate(q, carry):
        cols = [column(2, q * PART + k) for k in range(PART)]
        for k in range(PART):
            part = jnp.sum(cols[k] * column(1, q * PART + k), axis=0, keepdims=True)
            part = jnp.sum(part, axis=1, keepdims=True)
            gs[...] += jnp.where(lane == q * PART + k, part * scale, 0.0)
        spec = forward(cols, lead, twist, ahead)
        pairs = []
        for k in range(PART):
            spectra[2, q * PART + k] = spec[k]
            pairs.append(conj_times(pair_of(spectra[0, q * PART + k]), pair_of(spec[k])))
        for k, value in enumerate(inverse(pairs, trail, twist, back)):
            fs[q, pl.ds(k, SEQ, stride=PART), :] = value
        return carry

    lax.fori_loop(0, GROUPS, correlate, 0)
    for q in range(GROUPS):
        terms[q] = (fs[q] * scale).astype(BF16)
    swapped = [
        push(terms.at[2 * h + (1 - core)], near_in.at[h], sems(10 + h), {"chan": beside})
        for h in range(2)
    ]

    def through_of(q, carry):
        pairs = []
        for k in range(PART):
            j = q * PART + k
            pairs.append(conj_times(pair_of(spectra[1, j]), pair_of(spectra[2, j])))
        for k, value in enumerate(inverse(pairs, trail, twist, back)):
            put(2, q * PART + k, value)
        return carry

    lax.fori_loop(0, GROUPS, through_of, 0)
    for copy in swapped:
        copy.wait_recv()
    fs[0] = terms[group].astype(F32) + near_in[half].astype(F32)
    fs[1] = terms[across].astype(F32) + near_in[1 - half].astype(F32)

    def cut(s):
        for n in range(2):
            out_f[n, s] = fs[n, pl.ds(s * PART, PART), :].astype(BF16)

    in_steps(cut)

    def own_terms(peer):
        push(out_f.at[0, peer], rf.at[0, me], sems(12), {"seq": peer})
        push(gs, rs.at[me], sems(14), {"seq": peer})

    every_peer(
        me,
        lambda peer: push(
            out_f.at[1, peer], rf.at[1, me], sems(13), {"seq": peer, "chan": across}
        ),
        True,
    )
    every_peer(me, own_terms)
    rf[0, me] = out_f[0, me]
    rs[me] = gs[...]
    send_back(2)

    widen(0)

    def first(q, carry):
        cols = [column(0, q * PART + k) for k in range(PART)]
        spec = forward(cols, lead, twist, ahead)
        pairs = [
            times(pair_of(spectra[1, q * PART + k]), pair_of(spec[k])) for k in range(PART)
        ]
        for k, value in enumerate(inverse(pairs, trail, twist, back)):
            put(0, q * PART + k, value)
        return carry

    lax.fori_loop(0, GROUPS, first, 0)
    send_back(0)

    def unpack(m):
        waiting(most(r.at[m]), 3 + m).wait_recv()

        def one(peer):
            xs[m, pl.ds(peer, HELD, stride=SEQ), :] = r[m, peer].astype(F32)

        in_steps(one)

    def product(left, right):
        return (left.astype(F32) * right.astype(F32)).astype(BF16).astype(F32)

    blocks = [slice(b * ROWS, (b + 1) * ROWS) for b in range(WIDTH // ROWS)]
    unpack(1)
    for cols in blocks:
        mixed = xs[1, cols, :].T + skip[:, cols] * product(bk[:, cols], bv[:, cols])
        gq[:, cols] = (bg[:, cols].astype(F32) * mixed).astype(BF16)
    unpack(2)
    for cols in blocks:
        through = xs[2, cols, :].T + skip[:, cols] * product(bg[:, cols], bq[:, cols])
        gk[:, cols] = (through * bv[:, cols].astype(F32)).astype(BF16)
        gv[:, cols] = (through * bk[:, cols].astype(F32)).astype(BF16)
    last = [waiting(most(rf.at[0]), 12), waiting(rf.at[1], 13), waiting(most(rs), 14)]
    for copy in last:
        copy.wait_recv()
    ss[...] = jnp.zeros_like(ss)

    def unpack_terms(peer):
        fs[0, pl.ds(peer, PART, stride=SEQ), :] = rf[0, peer].astype(F32) + rf[1, peer].astype(F32)
        ss[pl.ds(peer, 1), :] = rs[peer]

    in_steps(unpack_terms)
    for cols in blocks[: QUARTER // ROWS]:
        gf[:, cols] = fs[0, cols, :].T
    ss[...] = ss[...].T
    even, odd = ss[pl.ds(0, 8, stride=2), :], ss[pl.ds(1, 8, stride=2), :]
    wide = lax.broadcasted_iota(jnp.int32, (8, ROWS), 1)
    gsk[...] = jnp.where(wide < SEQ, even, pltpu.roll(odd, SEQ, 1))
    unpack(0)
    for cols in blocks:
        mixed = xs[0, cols, :].T + skip[:, cols] * product(fk[:, cols], fv[:, cols])
        out[:, cols] = (fq[:, cols].astype(F32) * mixed).astype(BF16)
    for m in range(3):
        waiting(most(send.at[m]), m).wait_send()
        waiting(most(r.at[m]), 3 + m).wait_send()
    waiting(most(send_f), 6).wait_send()
    waiting(send_f, 7).wait_send()
    for copy in moved + swapped + last:
        copy.wait_send()


def exchange(fl, bk, bv, bg, bq, fk, fv, fq, skip):
    values = (fl, bk, bv, bg, bq, fk, fv, *[jnp.asarray(t) for t in tables()], fq, skip)
    wide = pltpu.VMEM((ROWS, WIDTH), BF16)
    return pl.pallas_call(
        main_kernel,
        out_shape=(
            wide,
            wide,
            wide,
            wide,
            pltpu.VMEM((ROWS, QUARTER), F32),
            pltpu.VMEM((8, ROWS), F32),
        ),
        in_specs=[pl.BlockSpec(memory_space=pltpu.HBM)] * COPIED,
        out_specs=[pl.BlockSpec(memory_space=pltpu.VMEM)] * 6,
        scratch_shapes=[
            *[pltpu.VMEM(v.shape, v.dtype) for v in values],
            pltpu.SemaphoreType.DMA((COPIED,)),
            pltpu.VMEM((3, SEQ, HELD, ROWS), BF16),
            pltpu.VMEM((2, SEQ, PART, ROWS), BF16),
            pltpu.VMEM((SEQ, 1, ROWS), F32),
            pltpu.VMEM((3, SEQ, HELD, ROWS), BF16),
            pltpu.VMEM((SEQ, PART, ROWS), BF16),
            pltpu.VMEM((3, SEQ, HELD, ROWS), BF16),
            pltpu.VMEM((GROUPS, SEQ, PART, ROWS), BF16),
            pltpu.VMEM((4, WIDTH, ROWS), F32),
            pltpu.VMEM((GROUPS, QUARTER, ROWS), F32),
            pltpu.VMEM((ROWS, ROWS), F32),
            pltpu.VMEM((3, HELD, SEQ, 2 * ROWS), F32),
            pltpu.VMEM((3, SEQ, HELD, ROWS), BF16),
            pltpu.VMEM((GROUPS, QUARTER, ROWS), BF16),
            pltpu.VMEM((2, QUARTER, ROWS), BF16),
            pltpu.VMEM((2, SEQ, PART, ROWS), BF16),
            pltpu.VMEM((1, ROWS), F32),
            pltpu.SemaphoreType.DMA((15,)),
            pltpu.SemaphoreType.DMA((15,)),
            pltpu.SemaphoreType.REGULAR,
        ],
        compiler_params=pltpu.CompilerParams(collective_id=0, has_side_effects=True),
    )(*values)


def store_kernel(*refs):
    count = len(refs) // 2
    sems = refs[-1]
    copies = [
        pltpu.make_async_copy(refs[n], refs[count + n], sems.at[n]) for n in range(count)
    ]
    for copy in copies:
        copy.start()
    for copy in copies:
        copy.wait()


def store(values):
    return pl.pallas_call(
        store_kernel,
        out_shape=tuple(jax.ShapeDtypeStruct(v.shape, v.dtype) for v in values),
        in_specs=[pl.BlockSpec(memory_space=pltpu.VMEM)] * len(values),
        out_specs=[pl.BlockSpec(memory_space=pl.ANY)] * len(values),
        scratch_shapes=[pltpu.SemaphoreType.DMA((len(values),))],
    )(*[pltpu.with_memory_space_constraint(v, pltpu.VMEM) for v in values])


def per_device(fwd_q, fwd_k, fwd_v, bwd_q, bwd_k, bwd_v, bwd_grad, filters, skip):
    done = exchange(
        filters, bwd_k, bwd_v, bwd_grad, bwd_q, fwd_k, fwd_v, fwd_q, skip[None, :]
    )
    *wide, skips = store(done)
    return (*wide, skips.reshape(WIDTH))


def solution(mesh):
    both = P("seq", "chan")
    return jax.shard_map(
        per_device,
        mesh=mesh,
        in_specs=(both,) * 8 + (P("chan"),),
        out_specs=(both,) * 5 + (P("chan"),),
        check_vma=False,
    )
```

```python
import functools
import math

import jax
import jax.numpy as jnp
import numpy as np
from jax import lax
from jax.experimental import pallas as pl
from jax.experimental.pallas import tpu as pltpu
from jax.sharding import PartitionSpec as P

MESH = pl.DeviceIdType.MESH
F32 = jnp.float32
BF16 = jnp.bfloat16
ROWS = 128
SEQ = 64
HELD = 16
GROUPS = 4
PART = HELD // GROUPS
TOTAL = ROWS * SEQ
WIDTH = SEQ * HELD
QUARTER = SEQ * PART
UNROLL = 2
COPIED = 14
DATA_LOW = True
TABLE_LOW = True


def halves(table):
    high = np.asarray(table, np.float32).astype(BF16)
    low = (np.asarray(table, np.float64) - high.astype(np.float64)).astype(np.float32).astype(BF16)
    return high, low


@functools.cache
def tables():
    row = np.arange(SEQ)
    lane = np.arange(ROWS)
    coarse = 2 * np.pi * ((row[None, :] * (4 * row[:, None] + 1)) % (4 * SEQ)) / (4 * SEQ)
    lead = np.concatenate([np.cos(coarse), -np.sin(coarse)], axis=0)
    lead = np.concatenate(halves(lead), axis=1)
    trail = np.concatenate([np.cos(coarse.T), -np.sin(coarse.T)], axis=1) / TOTAL
    trail = np.concatenate(halves(trail), axis=1)
    mid = 2 * np.pi * lane[None, :] * (4 * row[:, None] + 1) / (4 * TOTAL)
    twist = np.stack([np.cos(mid), np.sin(mid)]).astype(np.float32)
    fine = 2 * np.pi * ((lane[:, None] * lane[None, :]) % ROWS) / ROWS
    cosine, sine = np.cos(fine), np.sin(fine)
    ahead = np.stack(halves(np.block([[cosine, -sine], [sine, cosine]])))
    back = np.stack(halves(np.block([[cosine, sine], [-sine, cosine]])))
    return lead, trail, twist, ahead, back


def dot(left, right):
    return jnp.dot(left, right, preferred_element_type=F32)


def split_dot(values, table):
    high = values.astype(BF16)
    total = dot(high, table[0])
    if DATA_LOW:
        total += dot((values - high.astype(F32)).astype(BF16), table[0])
    if TABLE_LOW:
        total += dot(high, table[1])
    return total


def times(a, b):
    return a[0] * b[0] - a[1] * b[1], a[0] * b[1] + a[1] * b[0]


def conj_times(a, b):
    return a[0] * b[0] + a[1] * b[1], a[0] * b[1] - a[1] * b[0]


def forward(cols, lead, twist, ahead):
    x = jnp.concatenate(cols, axis=1).astype(BF16)
    front = dot(lead[...], jnp.concatenate([x, x], axis=0))
    rows = []
    for m in range(len(cols)):
        real, imag = front[:SEQ, m * ROWS : (m + 1) * ROWS], front[SEQ:, m * ROWS : (m + 1) * ROWS]
        turned = [real * twist[0] + imag * twist[1], imag * twist[0] - real * twist[1]]
        rows.append(jnp.concatenate(turned, axis=1))
    spec = split_dot(jnp.concatenate(rows, axis=0), ahead)
    return [spec[m * SEQ : (m + 1) * SEQ] for m in range(len(cols))]


def inverse(pairs, trail, twist, back):
    rows = jnp.concatenate([jnp.concatenate(pair, axis=1) for pair in pairs], axis=0)
    rows = split_dot(rows, back)
    reals, imags = [], []
    for m in range(len(pairs)):
        real, imag = rows[m * SEQ : (m + 1) * SEQ, :ROWS], rows[m * SEQ : (m + 1) * SEQ, ROWS:]
        reals.append(real * twist[0] - imag * twist[1])
        imags.append(real * twist[1] + imag * twist[0])
    z = jnp.concatenate([jnp.concatenate(reals, axis=1), jnp.concatenate(imags, axis=1)], axis=0)
    high = z.astype(BF16)
    final = dot(trail[...], jnp.concatenate([high, high], axis=0))
    if DATA_LOW:
        final += dot(trail[:, : 2 * SEQ], (z - high.astype(F32)).astype(BF16))
    return [final[:, m * ROWS : (m + 1) * ROWS] for m in range(len(pairs))]


def pair_of(spec):
    return spec[:, :ROWS], spec[:, ROWS:]


def rows_of(s, count):
    return pl.ds(pl.multiple_of(s * count, count), count)


def in_steps(body):
    def step(n, carry):
        for k in range(8):
            body(n * 8 + k)
        return carry

    lax.fori_loop(0, SEQ // 8, step, 0)


def owner(seq, half):
    x, z, y = seq // 16, (seq // 4) % 4, seq % 4
    return x * 16 + (z + half * (3 - 2 * z)) * 4 + y


def every_peer(me, half, body, flat=False):
    x, z, y = me // 16, (me // 4) % 4, me % 4
    ys = [(y + d) % 4 for d in (2, 1, 3, 0)]

    def row(dx, other, count):
        base = ((x + dx) % 4) * 16
        owned = other + half * (3 - 2 * other)
        for y_other in ys[:count]:
            body(base + other * 4 + y_other, base + owned * 4 + y_other)

    def rows(other, first):
        if flat:
            for dx in range(first, 4):
                row(dx, other, 4)
            return

        def one(dx, carry):
            row(dx, other, 4)
            return carry

        lax.fori_loop(first, 4, one, 0)

    for other in (3 - z, (z + 2) % 4, z + 1 - 2 * (z % 2)):
        rows(other, 0)
    rows(z, 1)
    row(0, z, 3)


def push(src, dst, sems, target):
    copy = pltpu.make_async_remote_copy(
        src_ref=src,
        dst_ref=dst,
        send_sem=sems[0],
        recv_sem=sems[1],
        device_id=target,
        device_id_type=MESH,
    )
    copy.start()
    return copy


def main_kernel(*refs):
    sources, (out, gq, gk, gv, gf, gsk) = refs[:COPIED], refs[COPIED : COPIED + 6]
    copied, loaded = refs[COPIED + 6 : 2 * COPIED + 6], refs[2 * COPIED + 6]
    (
        r, rf, rs, send, send_f, recv, filt, xs, fs, ss, spectra, y, terms, near_in, far_out,
        far_in, out_f, gs, gs_line, sent, got, ready,
    ) = refs[2 * COPIED + 7 :]
    fl, bk, bv, bg, bq, fk, fv, lead, trail, twist, ahead, back, fq, skip = copied
    me, group = lax.axis_index("seq"), lax.axis_index("chan")
    core, half = group % 2, group // 2
    beside, across = 2 * half + (1 - core), 2 * (1 - half) + core
    me_x, me_z, me_y = me // 16, (me // 4) % 4, me % 4
    mirror = {"seq": me_x * 16 + (3 - me_z) * 4 + me_y, "chan": across}
    mine = owner(me, half)
    barrier = pltpu.get_barrier_semaphore()
    loads = [
        pltpu.make_async_copy(sources[n], copied[n], loaded.at[n]) for n in range(COPIED)
    ]
    for load in loads:
        load.start()

    def hello(target, sem=barrier):
        pl.semaphore_signal(sem, inc=1, device_id=target, device_id_type=MESH)

    every_peer(me, half, lambda peer, _: hello({"seq": peer}), True)
    hello({"chan": beside})

    @pl.when(half == 0)
    def _():
        hello(mirror)

    def sems(n):
        return sent.at[n], got.at[n]

    def waiting(ref, n):
        return pltpu.make_async_remote_copy(
            src_ref=ref,
            dst_ref=ref,
            send_sem=sent.at[n],
            recv_sem=got.at[n],
            device_id={"chan": beside},
            device_id_type=MESH,
        )

    def most(ref):
        return ref.at[pl.ds(0, SEQ - 1)]

    def pack(m, left, right):
        for b in range(WIDTH // ROWS):
            cols = slice(b * ROWS, (b + 1) * ROWS)
            xs[m, cols, :] = (left[:, cols].astype(F32) * right[:, cols].astype(F32)).T

        def one(peer):
            send[m, peer] = xs[m, pl.ds(peer, HELD, stride=SEQ), :].astype(BF16)

        in_steps(one)

    def send_signal(m):
        every_peer(
            me,
            half,
            lambda peer, own: push(send.at[m, own], recv.at[m, me], sems(m), {"seq": peer}),
        )
        recv[m, me] = send[m, mine]

    def widen(m):
        waiting(most(recv.at[m]), m).wait_recv()

        def one(s):
            xs[m, rows_of(s, HELD), :] = recv[m, s].astype(F32)

        in_steps(one)

    def send_back(m, held):
        def one(s):
            y[m, s] = xs[held, rows_of(s, HELD), :].astype(BF16)

        in_steps(one)
        every_peer(
            me,
            half,
            lambda peer, _: push(y.at[m, peer], r.at[m, mine], sems(3 + m), {"seq": peer}),
        )
        r[m, mine] = y[m, me]

    loads[0].wait()
    for b in range(QUARTER // ROWS):
        cols = slice(b * ROWS, (b + 1) * ROWS)
        fs[0, cols, :] = fl[:, cols].T

    def filter_rows(peer):
        send_f[peer] = fs[0, pl.ds(peer, PART, stride=SEQ), :].astype(BF16)

    in_steps(filter_rows)
    loads[1].wait()
    loads[2].wait()
    pack(1, bk, bv)

    def pack_loaded(m, left, right, n):
        loads[n].wait()
        loads[n + 1].wait()
        pack(m, left, right)

    pl.semaphore_wait(barrier, SEQ + half)

    @pl.when(half == 1)
    def _():
        hello(mirror, ready)

    every_peer(
        me,
        half,
        lambda peer, own: push(send_f.at[own], filt.at[group, me], sems(6), {"seq": peer}),
    )
    filt[group, me] = send_f[mine]
    send_signal(1)
    pack_loaded(2, bg, bq, 3)
    send_signal(2)
    pack_loaded(0, fk, fv, 5)

    @pl.when(half == 0)
    def _():
        pl.semaphore_wait(ready, 1)

    waiting(most(filt.at[group]), 6).wait_recv()
    whole = filt.at[group]
    moved = [push(whole, whole, sems(7), mirror), push(whole, whole, sems(8), {"chan": beside})]
    send_signal(0)
    for load in loads[7:]:
        load.wait()
    moved[0].wait_recv()
    whole = filt.at[across]
    moved.append(push(whole, whole, sems(9), {"chan": beside}))

    def filter_wide(s):
        for q in range(GROUPS):
            fs[q, pl.ds(s * PART, PART), :] = filt[q, s].astype(F32)

    def column(m, j):
        return xs[m, pl.ds(j, SEQ, stride=HELD), :]

    def put(m, j, value):
        xs[m, pl.ds(j, SEQ, stride=HELD), :] = value

    widen(1)

    def second_ahead(q, carry):
        cols = [column(1, q * PART + k) for k in range(PART)]
        for k, spec in enumerate(forward(cols, lead, twist, ahead)):
            spectra[0, q * PART + k] = spec
        return carry

    lax.fori_loop(0, GROUPS, second_ahead, 0, unroll=UNROLL)
    for copy in moved[1:]:
        copy.wait_recv()
    in_steps(filter_wide)

    def second(q, carry):
        cols = [fs[q, pl.ds(k, SEQ, stride=PART), :] for k in range(PART)]
        pairs = []
        for k, spec in enumerate(forward(cols, lead, twist, ahead)):
            spectra[1, q * PART + k] = spec
            pairs.append(times(pair_of(spec), pair_of(spectra[0, q * PART + k])))
        for k, value in enumerate(inverse(pairs, trail, twist, back)):
            put(3, q * PART + k, value)
        return carry

    lax.fori_loop(0, GROUPS, second, 0, unroll=UNROLL)
    send_back(1, 3)

    widen(2)
    gs[...] = jnp.zeros_like(gs)
    lane = lax.broadcasted_iota(jnp.int32, (1, ROWS), 1)
    scale = 1.0 / math.sqrt(TOTAL)

    def correlate(q, carry):
        cols = [column(2, q * PART + k) for k in range(PART)]
        for k in range(PART):
            part = jnp.sum(cols[k] * column(1, q * PART + k), axis=0, keepdims=True)
            part = jnp.sum(part, axis=1, keepdims=True)
            gs[...] += jnp.where(lane == q * PART + k, part * scale, 0.0)
        spec = forward(cols, lead, twist, ahead)
        pairs = []
        for k in range(PART):
            spectra[2, q * PART + k] = spec[k]
            pairs.append(conj_times(pair_of(spectra[0, q * PART + k]), pair_of(spec[k])))
        for k, value in enumerate(inverse(pairs, trail, twist, back)):
            fs[q, pl.ds(k, SEQ, stride=PART), :] = value
        return carry

    lax.fori_loop(0, GROUPS, correlate, 0, unroll=UNROLL)
    for q in range(GROUPS):
        terms[q] = (fs[q] * scale).astype(BF16)
    swapped = [
        push(terms.at[2 * h + (1 - core)], near_in.at[h], sems(10 + h), {"chan": beside})
        for h in range(2)
    ]

    def through_of(q, carry):
        pairs = []
        for k in range(PART):
            j = q * PART + k
            pairs.append(conj_times(pair_of(spectra[1, j]), pair_of(spectra[2, j])))
        for k, value in enumerate(inverse(pairs, trail, twist, back)):
            put(2, q * PART + k, value)
        return carry

    lax.fori_loop(0, GROUPS, through_of, 0, unroll=UNROLL)
    for copy in swapped:
        copy.wait_recv()
    far_out[...] = (terms[across].astype(F32) + near_in[1 - half].astype(F32)).astype(BF16)
    far = push(far_out, far_in, sems(13), mirror)
    line = [
        push(gs, gs_line.at[mine // 4 % 4], sems(14), {"seq": me_x * 16 + other * 4 + me_y})
        for other in (3 - me_z, (me_z + 2) % 4, me_z + 1 - 2 * (me_z % 2))
    ]
    gs_line[mine // 4 % 4] = gs[...]
    fs[0] = terms[group].astype(F32) + near_in[half].astype(F32)
    send_back(2, 2)

    widen(0)

    def first(q, carry):
        cols = [column(0, q * PART + k) for k in range(PART)]
        spec = forward(cols, lead, twist, ahead)
        pairs = [
            times(pair_of(spectra[1, q * PART + k]), pair_of(spec[k])) for k in range(PART)
        ]
        for k, value in enumerate(inverse(pairs, trail, twist, back)):
            put(0, q * PART + k, value)
        return carry

    lax.fori_loop(0, GROUPS, first, 0, unroll=UNROLL)
    far.wait_recv()
    fs[0] += far_in[...].astype(F32)

    def cut(s):
        out_f[s] = fs[0, pl.ds(s * PART, PART), :].astype(BF16)

    in_steps(cut)
    every_peer(
        me,
        half,
        lambda peer, _: push(out_f.at[peer], rf.at[mine], sems(12), {"seq": peer}),
    )
    rf[mine] = out_f[me]
    whole_line = waiting(gs_line.at[pl.ds(0, 3)], 14)
    whole_line.wait_recv()

    def plane(dx, carry):
        for d in range(4):
            peer = ((me_x + dx) % 4) * 16 + me_z * 4 + (me_y + d) % 4
            push(gs_line, rs.at[me_x * 4 + me_y], sems(15), {"seq": peer})
        return carry

    lax.fori_loop(1, 4, plane, 0)
    for d in range(1, 4):
        peer = me_x * 16 + me_z * 4 + (me_y + d) % 4
        push(gs_line, rs.at[me_x * 4 + me_y], sems(15), {"seq": peer})
    rs[me_x * 4 + me_y] = gs_line[...]
    send_back(0, 0)

    def unpack(m):
        waiting(most(r.at[m]), 3 + m).wait_recv()

        def one(peer):
            xs[m, pl.ds(peer, HELD, stride=SEQ), :] = r[m, peer].astype(F32)

        in_steps(one)

    def product(left, right):
        return (left.astype(F32) * right.astype(F32)).astype(BF16).astype(F32)

    blocks = [slice(b * ROWS, (b + 1) * ROWS) for b in range(WIDTH // ROWS)]
    unpack(1)
    for cols in blocks:
        mixed = xs[1, cols, :].T + skip[:, cols] * product(bk[:, cols], bv[:, cols])
        gq[:, cols] = (bg[:, cols].astype(F32) * mixed).astype(BF16)
    unpack(2)
    for cols in blocks:
        through = xs[2, cols, :].T + skip[:, cols] * product(bg[:, cols], bq[:, cols])
        gk[:, cols] = (through * bv[:, cols].astype(F32)).astype(BF16)
        gv[:, cols] = (through * bk[:, cols].astype(F32)).astype(BF16)
    last = [waiting(most(rf), 12), waiting(rs.at[pl.ds(0, 15)], 15)]
    for copy in last:
        copy.wait_recv()
    ss[...] = jnp.zeros_like(ss)

    def unpack_terms(p):
        fs[0, pl.ds(p, PART, stride=SEQ), :] = rf[p].astype(F32)

    in_steps(unpack_terms)
    for p in range(SEQ):
        ss[p : p + 1, :] = rs[(p // 16) * 4 + p % 4, (p // 4) % 4]
    for cols in blocks[: QUARTER // ROWS]:
        gf[:, cols] = fs[0, cols, :].T
    ss[...] = ss[...].T
    even, odd = ss[pl.ds(0, 8, stride=2), :], ss[pl.ds(1, 8, stride=2), :]
    wide = lax.broadcasted_iota(jnp.int32, (8, ROWS), 1)
    gsk[...] = jnp.where(wide < SEQ, even, pltpu.roll(odd, SEQ, 1))
    unpack(0)
    for cols in blocks:
        mixed = xs[0, cols, :].T + skip[:, cols] * product(fk[:, cols], fv[:, cols])
        out[:, cols] = (fq[:, cols].astype(F32) * mixed).astype(BF16)
    for m in range(3):
        waiting(most(send.at[m]), m).wait_send()
        waiting(most(r.at[m]), 3 + m).wait_send()
    waiting(most(send_f), 6).wait_send()
    for copy in [*moved, *swapped, far, whole_line, *last]:
        copy.wait_send()


def exchange(fl, bk, bv, bg, bq, fk, fv, fq, skip):
    values = (fl, bk, bv, bg, bq, fk, fv, *[jnp.asarray(t) for t in tables()], fq, skip)
    wide = pltpu.VMEM((ROWS, WIDTH), BF16)
    return pl.pallas_call(
        main_kernel,
        out_shape=(
            wide,
            wide,
            wide,
            wide,
            pltpu.VMEM((ROWS, QUARTER), F32),
            pltpu.VMEM((8, ROWS), F32),
        ),
        in_specs=[pl.BlockSpec(memory_space=pltpu.HBM)] * COPIED,
        out_specs=[pl.BlockSpec(memory_space=pltpu.VMEM)] * 6,
        scratch_shapes=[
            *[pltpu.VMEM(v.shape, v.dtype) for v in values],
            pltpu.SemaphoreType.DMA((COPIED,)),
            pltpu.VMEM((3, SEQ, HELD, ROWS), BF16),
            pltpu.VMEM((SEQ, PART, ROWS), BF16),
            pltpu.VMEM((16, 4, 1, ROWS), F32),
            pltpu.VMEM((3, SEQ, HELD, ROWS), BF16),
            pltpu.VMEM((SEQ, PART, ROWS), BF16),
            pltpu.VMEM((3, SEQ, HELD, ROWS), BF16),
            pltpu.VMEM((GROUPS, SEQ, PART, ROWS), BF16),
            pltpu.VMEM((4, WIDTH, ROWS), F32),
            pltpu.VMEM((GROUPS, QUARTER, ROWS), F32),
            pltpu.VMEM((ROWS, ROWS), F32),
            pltpu.VMEM((3, HELD, SEQ, 2 * ROWS), F32),
            pltpu.VMEM((3, SEQ, HELD, ROWS), BF16),
            pltpu.VMEM((GROUPS, QUARTER, ROWS), BF16),
            pltpu.VMEM((2, QUARTER, ROWS), BF16),
            pltpu.VMEM((QUARTER, ROWS), BF16),
            pltpu.VMEM((QUARTER, ROWS), BF16),
            pltpu.VMEM((SEQ, PART, ROWS), BF16),
            pltpu.VMEM((1, ROWS), F32),
            pltpu.VMEM((4, 1, ROWS), F32),
            pltpu.SemaphoreType.DMA((16,)),
            pltpu.SemaphoreType.DMA((16,)),
            pltpu.SemaphoreType.REGULAR,
        ],
        compiler_params=pltpu.CompilerParams(collective_id=0, has_side_effects=True),
    )(*values)


def store_kernel(*refs):
    count = len(refs) // 2
    sems = refs[-1]
    copies = [
        pltpu.make_async_copy(refs[n], refs[count + n], sems.at[n]) for n in range(count)
    ]
    for copy in copies:
        copy.start()
    for copy in copies:
        copy.wait()


def store(values):
    return pl.pallas_call(
        store_kernel,
        out_shape=tuple(jax.ShapeDtypeStruct(v.shape, v.dtype) for v in values),
        in_specs=[pl.BlockSpec(memory_space=pltpu.VMEM)] * len(values),
        out_specs=[pl.BlockSpec(memory_space=pl.ANY)] * len(values),
        scratch_shapes=[pltpu.SemaphoreType.DMA((len(values),))],
    )(*[pltpu.with_memory_space_constraint(v, pltpu.VMEM) for v in values])


def per_device(fwd_q, fwd_k, fwd_v, bwd_q, bwd_k, bwd_v, bwd_grad, filters, skip):
    done = exchange(
        filters, bwd_k, bwd_v, bwd_grad, bwd_q, fwd_k, fwd_v, fwd_q, skip[None, :]
    )
    *wide, skips = store(done)
    return (*wide, skips.reshape(WIDTH))


def solution(mesh):
    both = P("seq", "chan")
    return jax.shard_map(
        per_device,
        mesh=mesh,
        in_specs=(both,) * 8 + (P("chan"),),
        out_specs=(both,) * 5 + (P("chan"),),
        check_vma=False,
    )
```

```python
import functools
import math

import jax
import jax.numpy as jnp
import numpy as np
from jax import lax
from jax.experimental import pallas as pl
from jax.experimental.pallas import tpu as pltpu
from jax.sharding import PartitionSpec as P

MESH = pl.DeviceIdType.MESH
F32 = jnp.float32
BF16 = jnp.bfloat16
ROWS = 128
SEQ = 64
HELD = 16
GROUPS = 4
PART = HELD // GROUPS
TOTAL = ROWS * SEQ
WIDTH = SEQ * HELD
QUARTER = SEQ * PART
UNROLL = 2
COPIED = 14
DATA_LOW = False
TABLE_LOW = True


def halves(table):
    high = np.asarray(table, np.float32).astype(BF16)
    low = (np.asarray(table, np.float64) - high.astype(np.float64)).astype(np.float32).astype(BF16)
    return high, low


@functools.cache
def tables():
    row = np.arange(SEQ)
    lane = np.arange(ROWS)
    coarse = 2 * np.pi * ((row[None, :] * (4 * row[:, None] + 1)) % (4 * SEQ)) / (4 * SEQ)
    lead = np.concatenate([np.cos(coarse), -np.sin(coarse)], axis=0)
    lead = np.concatenate(halves(lead), axis=1)
    trail = np.concatenate([np.cos(coarse.T), -np.sin(coarse.T)], axis=1) / TOTAL
    trail = np.concatenate(halves(trail), axis=1)
    mid = 2 * np.pi * lane[None, :] * (4 * row[:, None] + 1) / (4 * TOTAL)
    twist = np.stack([np.cos(mid), np.sin(mid)]).astype(np.float32)
    fine = 2 * np.pi * ((lane[:, None] * lane[None, :]) % ROWS) / ROWS
    cosine, sine = np.cos(fine), np.sin(fine)
    ahead = np.stack(halves(np.block([[cosine, -sine], [sine, cosine]])))
    back = np.stack(halves(np.block([[cosine, sine], [-sine, cosine]])))
    return lead, trail, twist, ahead, back


def dot(left, right):
    return jnp.dot(left, right, preferred_element_type=F32)


def split_dot(values, table):
    high = values.astype(BF16)
    total = dot(high, table[0])
    if DATA_LOW:
        total += dot((values - high.astype(F32)).astype(BF16), table[0])
    if TABLE_LOW:
        total += dot(high, table[1])
    return total


def times(a, b):
    return a[0] * b[0] - a[1] * b[1], a[0] * b[1] + a[1] * b[0]


def conj_times(a, b):
    return a[0] * b[0] + a[1] * b[1], a[0] * b[1] - a[1] * b[0]


def forward(cols, lead, twist, ahead):
    x = jnp.concatenate(cols, axis=1).astype(BF16)
    front = dot(lead[...], jnp.concatenate([x, x], axis=0))
    rows = []
    for m in range(len(cols)):
        real, imag = front[:SEQ, m * ROWS : (m + 1) * ROWS], front[SEQ:, m * ROWS : (m + 1) * ROWS]
        turned = [real * twist[0] + imag * twist[1], imag * twist[0] - real * twist[1]]
        rows.append(jnp.concatenate(turned, axis=1))
    spec = split_dot(jnp.concatenate(rows, axis=0), ahead)
    return [spec[m * SEQ : (m + 1) * SEQ] for m in range(len(cols))]


def inverse(pairs, trail, twist, back):
    rows = jnp.concatenate([jnp.concatenate(pair, axis=1) for pair in pairs], axis=0)
    rows = split_dot(rows, back)
    reals, imags = [], []
    for m in range(len(pairs)):
        real, imag = rows[m * SEQ : (m + 1) * SEQ, :ROWS], rows[m * SEQ : (m + 1) * SEQ, ROWS:]
        reals.append(real * twist[0] - imag * twist[1])
        imags.append(real * twist[1] + imag * twist[0])
    z = jnp.concatenate([jnp.concatenate(reals, axis=1), jnp.concatenate(imags, axis=1)], axis=0)
    high = z.astype(BF16)
    final = dot(trail[...], jnp.concatenate([high, high], axis=0))
    if DATA_LOW:
        final += dot(trail[:, : 2 * SEQ], (z - high.astype(F32)).astype(BF16))
    return [final[:, m * ROWS : (m + 1) * ROWS] for m in range(len(pairs))]


def pair_of(spec):
    return spec[:, :ROWS], spec[:, ROWS:]


def rows_of(s, count):
    return pl.ds(pl.multiple_of(s * count, count), count)


def in_steps(body):
    def step(n, carry):
        for k in range(8):
            body(n * 8 + k)
        return carry

    lax.fori_loop(0, SEQ // 8, step, 0)


def owner(seq, half):
    x, z, y = seq // 16, (seq // 4) % 4, seq % 4
    return x * 16 + (z + half * (3 - 2 * z)) * 4 + y


def every_peer(me, half, body, flat=False):
    x, z, y = me // 16, (me // 4) % 4, me % 4
    ys = [(y + d) % 4 for d in (2, 1, 3, 0)]

    def row(dx, other, count):
        base = ((x + dx) % 4) * 16
        owned = other + half * (3 - 2 * other)
        for y_other in ys[:count]:
            body(base + other * 4 + y_other, base + owned * 4 + y_other)

    def rows(other, first):
        if flat:
            for dx in range(first, 4):
                row(dx, other, 4)
            return

        def one(dx, carry):
            row(dx, other, 4)
            return carry

        lax.fori_loop(first, 4, one, 0)

    for other in (3 - z, (z + 2) % 4, z + 1 - 2 * (z % 2)):
        rows(other, 0)
    rows(z, 1)
    row(0, z, 3)


def push(src, dst, sems, target):
    copy = pltpu.make_async_remote_copy(
        src_ref=src,
        dst_ref=dst,
        send_sem=sems[0],
        recv_sem=sems[1],
        device_id=target,
        device_id_type=MESH,
    )
    copy.start()
    return copy


def main_kernel(*refs):
    sources, (out, gq, gk, gv, gf, gsk) = refs[:COPIED], refs[COPIED : COPIED + 6]
    copied, loaded = refs[COPIED + 6 : 2 * COPIED + 6], refs[2 * COPIED + 6]
    (
        r, rf, rs, send, send_f, recv, filt, xs, fs, ss, spectra, y, terms, near_in, far_out,
        far_in, out_f, gs, gs_line, sent, got, ready,
    ) = refs[2 * COPIED + 7 :]
    fl, bk, bv, bg, bq, fk, fv, lead, trail, twist, ahead, back, fq, skip = copied
    me, group = lax.axis_index("seq"), lax.axis_index("chan")
    core, half = group % 2, group // 2
    beside, across = 2 * half + (1 - core), 2 * (1 - half) + core
    me_x, me_z, me_y = me // 16, (me // 4) % 4, me % 4
    mirror = {"seq": me_x * 16 + (3 - me_z) * 4 + me_y, "chan": across}
    mine = owner(me, half)
    barrier = pltpu.get_barrier_semaphore()
    loads = [
        pltpu.make_async_copy(sources[n], copied[n], loaded.at[n]) for n in range(COPIED)
    ]
    for load in loads:
        load.start()

    def hello(target, sem=barrier):
        pl.semaphore_signal(sem, inc=1, device_id=target, device_id_type=MESH)

    every_peer(me, half, lambda peer, _: hello({"seq": peer}), True)
    hello({"chan": beside})

    @pl.when(half == 0)
    def _():
        hello(mirror)

    def sems(n):
        return sent.at[n], got.at[n]

    def waiting(ref, n):
        return pltpu.make_async_remote_copy(
            src_ref=ref,
            dst_ref=ref,
            send_sem=sent.at[n],
            recv_sem=got.at[n],
            device_id={"chan": beside},
            device_id_type=MESH,
        )

    def most(ref):
        return ref.at[pl.ds(0, SEQ - 1)]

    def pack(m, left, right):
        for b in range(WIDTH // ROWS):
            cols = slice(b * ROWS, (b + 1) * ROWS)
            xs[m, cols, :] = (left[:, cols].astype(F32) * right[:, cols].astype(F32)).T

        def one(peer):
            send[m, peer] = xs[m, pl.ds(peer, HELD, stride=SEQ), :].astype(BF16)

        in_steps(one)

    def send_signal(m):
        every_peer(
            me,
            half,
            lambda peer, own: push(send.at[m, own], recv.at[m, me], sems(m), {"seq": peer}),
        )
        recv[m, me] = send[m, mine]

    def widen(m):
        waiting(most(recv.at[m]), m).wait_recv()

        def one(s):
            xs[m, rows_of(s, HELD), :] = recv[m, s].astype(F32)

        in_steps(one)

    def send_back(m, held):
        def one(s):
            y[m, s] = xs[held, rows_of(s, HELD), :].astype(BF16)

        in_steps(one)
        every_peer(
            me,
            half,
            lambda peer, _: push(y.at[m, peer], r.at[m, mine], sems(3 + m), {"seq": peer}),
        )
        r[m, mine] = y[m, me]

    loads[0].wait()
    for b in range(QUARTER // ROWS):
        cols = slice(b * ROWS, (b + 1) * ROWS)
        fs[0, cols, :] = fl[:, cols].T

    def filter_rows(peer):
        send_f[peer] = fs[0, pl.ds(peer, PART, stride=SEQ), :].astype(BF16)

    in_steps(filter_rows)
    loads[1].wait()
    loads[2].wait()
    pack(1, bk, bv)

    def pack_loaded(m, left, right, n):
        loads[n].wait()
        loads[n + 1].wait()
        pack(m, left, right)

    pl.semaphore_wait(barrier, SEQ + half)

    @pl.when(half == 1)
    def _():
        hello(mirror, ready)

    every_peer(
        me,
        half,
        lambda peer, own: push(send_f.at[own], filt.at[group, me], sems(6), {"seq": peer}),
    )
    filt[group, me] = send_f[mine]
    send_signal(1)
    pack_loaded(2, bg, bq, 3)
    send_signal(2)
    pack_loaded(0, fk, fv, 5)

    @pl.when(half == 0)
    def _():
        pl.semaphore_wait(ready, 1)

    waiting(most(filt.at[group]), 6).wait_recv()
    whole = filt.at[group]
    moved = [push(whole, whole, sems(7), mirror), push(whole, whole, sems(8), {"chan": beside})]
    send_signal(0)
    for load in loads[7:]:
        load.wait()
    moved[0].wait_recv()
    whole = filt.at[across]
    moved.append(push(whole, whole, sems(9), {"chan": beside}))

    def filter_wide(s):
        for q in range(GROUPS):
            fs[q, pl.ds(s * PART, PART), :] = filt[q, s].astype(F32)

    def column(m, j):
        return xs[m, pl.ds(j, SEQ, stride=HELD), :]

    def put(m, j, value):
        xs[m, pl.ds(j, SEQ, stride=HELD), :] = value

    widen(1)

    def second_ahead(q, carry):
        cols = [column(1, q * PART + k) for k in range(PART)]
        for k, spec in enumerate(forward(cols, lead, twist, ahead)):
            spectra[0, q * PART + k] = spec
        return carry

    lax.fori_loop(0, GROUPS, second_ahead, 0, unroll=UNROLL)
    for copy in moved[1:]:
        copy.wait_recv()
    in_steps(filter_wide)

    def second(q, carry):
        cols = [fs[q, pl.ds(k, SEQ, stride=PART), :] for k in range(PART)]
        pairs = []
        for k, spec in enumerate(forward(cols, lead, twist, ahead)):
            spectra[1, q * PART + k] = spec
            pairs.append(times(pair_of(spec), pair_of(spectra[0, q * PART + k])))
        for k, value in enumerate(inverse(pairs, trail, twist, back)):
            put(3, q * PART + k, value)
        return carry

    lax.fori_loop(0, GROUPS, second, 0, unroll=UNROLL)
    send_back(1, 3)

    widen(2)
    gs[...] = jnp.zeros_like(gs)
    lane = lax.broadcasted_iota(jnp.int32, (1, ROWS), 1)
    scale = 1.0 / math.sqrt(TOTAL)

    def correlate(q, carry):
        cols = [column(2, q * PART + k) for k in range(PART)]
        for k in range(PART):
            part = jnp.sum(cols[k] * column(1, q * PART + k), axis=0, keepdims=True)
            part = jnp.sum(part, axis=1, keepdims=True)
            gs[...] += jnp.where(lane == q * PART + k, part * scale, 0.0)
        spec = forward(cols, lead, twist, ahead)
        pairs = []
        for k in range(PART):
            spectra[2, q * PART + k] = spec[k]
            pairs.append(conj_times(pair_of(spectra[0, q * PART + k]), pair_of(spec[k])))
        for k, value in enumerate(inverse(pairs, trail, twist, back)):
            fs[q, pl.ds(k, SEQ, stride=PART), :] = value
        return carry

    lax.fori_loop(0, GROUPS, correlate, 0, unroll=UNROLL)
    for q in range(GROUPS):
        terms[q] = (fs[q] * scale).astype(BF16)
    swapped = [
        push(terms.at[2 * h + (1 - core)], near_in.at[h], sems(10 + h), {"chan": beside})
        for h in range(2)
    ]

    def through_of(q, carry):
        pairs = []
        for k in range(PART):
            j = q * PART + k
            pairs.append(conj_times(pair_of(spectra[1, j]), pair_of(spectra[2, j])))
        for k, value in enumerate(inverse(pairs, trail, twist, back)):
            put(2, q * PART + k, value)
        return carry

    lax.fori_loop(0, GROUPS, through_of, 0, unroll=UNROLL)
    for copy in swapped:
        copy.wait_recv()
    far_out[...] = (terms[across].astype(F32) + near_in[1 - half].astype(F32)).astype(BF16)
    far = push(far_out, far_in, sems(13), mirror)
    line = [
        push(gs, gs_line.at[mine // 4 % 4], sems(14), {"seq": me_x * 16 + other * 4 + me_y})
        for other in (3 - me_z, (me_z + 2) % 4, me_z + 1 - 2 * (me_z % 2))
    ]
    gs_line[mine // 4 % 4] = gs[...]
    fs[0] = terms[group].astype(F32) + near_in[half].astype(F32)
    send_back(2, 2)

    widen(0)

    def first(q, carry):
        cols = [column(0, q * PART + k) for k in range(PART)]
        spec = forward(cols, lead, twist, ahead)
        pairs = [
            times(pair_of(spectra[1, q * PART + k]), pair_of(spec[k])) for k in range(PART)
        ]
        for k, value in enumerate(inverse(pairs, trail, twist, back)):
            put(0, q * PART + k, value)
        return carry

    lax.fori_loop(0, GROUPS, first, 0, unroll=UNROLL)
    far.wait_recv()
    fs[0] += far_in[...].astype(F32)

    def cut(s):
        out_f[s] = fs[0, pl.ds(s * PART, PART), :].astype(BF16)

    in_steps(cut)
    every_peer(
        me,
        half,
        lambda peer, _: push(out_f.at[peer], rf.at[mine], sems(12), {"seq": peer}),
    )
    rf[mine] = out_f[me]
    whole_line = waiting(gs_line.at[pl.ds(0, 3)], 14)
    whole_line.wait_recv()

    def plane(dx, carry):
        for d in range(4):
            peer = ((me_x + dx) % 4) * 16 + me_z * 4 + (me_y + d) % 4
            push(gs_line, rs.at[me_x * 4 + me_y], sems(15), {"seq": peer})
        return carry

    lax.fori_loop(1, 4, plane, 0)
    for d in range(1, 4):
        peer = me_x * 16 + me_z * 4 + (me_y + d) % 4
        push(gs_line, rs.at[me_x * 4 + me_y], sems(15), {"seq": peer})
    rs[me_x * 4 + me_y] = gs_line[...]
    send_back(0, 0)

    def unpack(m):
        waiting(most(r.at[m]), 3 + m).wait_recv()

        def one(peer):
            xs[m, pl.ds(peer, HELD, stride=SEQ), :] = r[m, peer].astype(F32)

        in_steps(one)

    def product(left, right):
        return (left.astype(F32) * right.astype(F32)).astype(BF16).astype(F32)

    blocks = [slice(b * ROWS, (b + 1) * ROWS) for b in range(WIDTH // ROWS)]
    unpack(1)
    for cols in blocks:
        mixed = xs[1, cols, :].T + skip[:, cols] * product(bk[:, cols], bv[:, cols])
        gq[:, cols] = (bg[:, cols].astype(F32) * mixed).astype(BF16)
    unpack(2)
    for cols in blocks:
        through = xs[2, cols, :].T + skip[:, cols] * product(bg[:, cols], bq[:, cols])
        gk[:, cols] = (through * bv[:, cols].astype(F32)).astype(BF16)
        gv[:, cols] = (through * bk[:, cols].astype(F32)).astype(BF16)
    last = [waiting(most(rf), 12), waiting(rs.at[pl.ds(0, 15)], 15)]
    for copy in last:
        copy.wait_recv()
    ss[...] = jnp.zeros_like(ss)

    def unpack_terms(p):
        fs[0, pl.ds(p, PART, stride=SEQ), :] = rf[p].astype(F32)

    in_steps(unpack_terms)
    for p in range(SEQ):
        ss[p : p + 1, :] = rs[(p // 16) * 4 + p % 4, (p // 4) % 4]
    for cols in blocks[: QUARTER // ROWS]:
        gf[:, cols] = fs[0, cols, :].T
    ss[...] = ss[...].T
    even, odd = ss[pl.ds(0, 8, stride=2), :], ss[pl.ds(1, 8, stride=2), :]
    wide = lax.broadcasted_iota(jnp.int32, (8, ROWS), 1)
    gsk[...] = jnp.where(wide < SEQ, even, pltpu.roll(odd, SEQ, 1))
    unpack(0)
    for cols in blocks:
        mixed = xs[0, cols, :].T + skip[:, cols] * product(fk[:, cols], fv[:, cols])
        out[:, cols] = (fq[:, cols].astype(F32) * mixed).astype(BF16)
    for m in range(3):
        waiting(most(send.at[m]), m).wait_send()
        waiting(most(r.at[m]), 3 + m).wait_send()
    waiting(most(send_f), 6).wait_send()
    for copy in [*moved, *swapped, far, whole_line, *last]:
        copy.wait_send()


def exchange(fl, bk, bv, bg, bq, fk, fv, fq, skip):
    values = (fl, bk, bv, bg, bq, fk, fv, *[jnp.asarray(t) for t in tables()], fq, skip)
    wide = pltpu.VMEM((ROWS, WIDTH), BF16)
    return pl.pallas_call(
        main_kernel,
        out_shape=(
            wide,
            wide,
            wide,
            wide,
            pltpu.VMEM((ROWS, QUARTER), F32),
            pltpu.VMEM((8, ROWS), F32),
        ),
        in_specs=[pl.BlockSpec(memory_space=pltpu.HBM)] * COPIED,
        out_specs=[pl.BlockSpec(memory_space=pltpu.VMEM)] * 6,
        scratch_shapes=[
            *[pltpu.VMEM(v.shape, v.dtype) for v in values],
            pltpu.SemaphoreType.DMA((COPIED,)),
            pltpu.VMEM((3, SEQ, HELD, ROWS), BF16),
            pltpu.VMEM((SEQ, PART, ROWS), BF16),
            pltpu.VMEM((16, 4, 1, ROWS), F32),
            pltpu.VMEM((3, SEQ, HELD, ROWS), BF16),
            pltpu.VMEM((SEQ, PART, ROWS), BF16),
            pltpu.VMEM((3, SEQ, HELD, ROWS), BF16),
            pltpu.VMEM((GROUPS, SEQ, PART, ROWS), BF16),
            pltpu.VMEM((4, WIDTH, ROWS), F32),
            pltpu.VMEM((GROUPS, QUARTER, ROWS), F32),
            pltpu.VMEM((ROWS, ROWS), F32),
            pltpu.VMEM((3, HELD, SEQ, 2 * ROWS), F32),
            pltpu.VMEM((3, SEQ, HELD, ROWS), BF16),
            pltpu.VMEM((GROUPS, QUARTER, ROWS), BF16),
            pltpu.VMEM((2, QUARTER, ROWS), BF16),
            pltpu.VMEM((QUARTER, ROWS), BF16),
            pltpu.VMEM((QUARTER, ROWS), BF16),
            pltpu.VMEM((SEQ, PART, ROWS), BF16),
            pltpu.VMEM((1, ROWS), F32),
            pltpu.VMEM((4, 1, ROWS), F32),
            pltpu.SemaphoreType.DMA((16,)),
            pltpu.SemaphoreType.DMA((16,)),
            pltpu.SemaphoreType.REGULAR,
        ],
        compiler_params=pltpu.CompilerParams(collective_id=0, has_side_effects=True),
    )(*values)


def store_kernel(*refs):
    count = len(refs) // 2
    sems = refs[-1]
    copies = [
        pltpu.make_async_copy(refs[n], refs[count + n], sems.at[n]) for n in range(count)
    ]
    for copy in copies:
        copy.start()
    for copy in copies:
        copy.wait()


def store(values):
    return pl.pallas_call(
        store_kernel,
        out_shape=tuple(jax.ShapeDtypeStruct(v.shape, v.dtype) for v in values),
        in_specs=[pl.BlockSpec(memory_space=pltpu.VMEM)] * len(values),
        out_specs=[pl.BlockSpec(memory_space=pl.ANY)] * len(values),
        scratch_shapes=[pltpu.SemaphoreType.DMA((len(values),))],
    )(*[pltpu.with_memory_space_constraint(v, pltpu.VMEM) for v in values])


def per_device(fwd_q, fwd_k, fwd_v, bwd_q, bwd_k, bwd_v, bwd_grad, filters, skip):
    done = exchange(
        filters, bwd_k, bwd_v, bwd_grad, bwd_q, fwd_k, fwd_v, fwd_q, skip[None, :]
    )
    *wide, skips = store(done)
    return (*wide, skips.reshape(WIDTH))


def solution(mesh):
    both = P("seq", "chan")
    return jax.shard_map(
        per_device,
        mesh=mesh,
        in_specs=(both,) * 8 + (P("chan"),),
        out_specs=(both,) * 5 + (P("chan"),),
        check_vma=False,
    )
```

```python
import functools
import math

import jax
import jax.numpy as jnp
import numpy as np
from jax import lax
from jax.experimental import pallas as pl
from jax.experimental.pallas import tpu as pltpu
from jax.sharding import PartitionSpec as P

MESH = pl.DeviceIdType.MESH
F32 = jnp.float32
BF16 = jnp.bfloat16
ROWS = 128
SEQ = 64
HELD = 16
GROUPS = 4
PART = HELD // GROUPS
TOTAL = ROWS * SEQ
WIDTH = SEQ * HELD
QUARTER = SEQ * PART
UNROLL = 4
COPIED = 14
DATA_LOW = False
TABLE_LOW = True


def halves(table):
    high = np.asarray(table, np.float32).astype(BF16)
    low = (np.asarray(table, np.float64) - high.astype(np.float64)).astype(np.float32).astype(BF16)
    return high, low


@functools.cache
def tables():
    row = np.arange(SEQ)
    lane = np.arange(ROWS)
    coarse = 2 * np.pi * ((row[None, :] * (4 * row[:, None] + 1)) % (4 * SEQ)) / (4 * SEQ)
    lead = np.concatenate([np.cos(coarse), -np.sin(coarse)], axis=0)
    lead = np.concatenate(halves(lead), axis=1)
    trail = np.concatenate([np.cos(coarse.T), -np.sin(coarse.T)], axis=1) / TOTAL
    trail = np.concatenate(halves(trail), axis=1)
    mid = 2 * np.pi * lane[None, :] * (4 * row[:, None] + 1) / (4 * TOTAL)
    twist = np.stack([np.cos(mid), np.sin(mid)]).astype(np.float32)
    fine = 2 * np.pi * ((lane[:, None] * lane[None, :]) % ROWS) / ROWS
    cosine, sine = np.cos(fine), np.sin(fine)
    ahead = np.stack(halves(np.block([[cosine, -sine], [sine, cosine]])))
    back = np.stack(halves(np.block([[cosine, sine], [-sine, cosine]])))
    return lead, trail, twist, ahead, back


def dot(left, right):
    return jnp.dot(left, right, preferred_element_type=F32)


def split_dot(values, table):
    high = values.astype(BF16)
    total = dot(high, table[0])
    if DATA_LOW:
        total += dot((values - high.astype(F32)).astype(BF16), table[0])
    if TABLE_LOW:
        total += dot(high, table[1])
    return total


def times(a, b):
    return a[0] * b[0] - a[1] * b[1], a[0] * b[1] + a[1] * b[0]


def conj_times(a, b):
    return a[0] * b[0] + a[1] * b[1], a[0] * b[1] - a[1] * b[0]


def forward(cols, lead, twist, ahead):
    x = jnp.concatenate(cols, axis=1).astype(BF16)
    front = dot(lead[...], jnp.concatenate([x, x], axis=0))
    rows = []
    for m in range(len(cols)):
        real, imag = front[:SEQ, m * ROWS : (m + 1) * ROWS], front[SEQ:, m * ROWS : (m + 1) * ROWS]
        turned = [real * twist[0] + imag * twist[1], imag * twist[0] - real * twist[1]]
        rows.append(jnp.concatenate(turned, axis=1))
    spec = split_dot(jnp.concatenate(rows, axis=0), ahead)
    return [spec[m * SEQ : (m + 1) * SEQ] for m in range(len(cols))]


def inverse(pairs, trail, twist, back):
    rows = jnp.concatenate([jnp.concatenate(pair, axis=1) for pair in pairs], axis=0)
    rows = split_dot(rows, back)
    reals, imags = [], []
    for m in range(len(pairs)):
        real, imag = rows[m * SEQ : (m + 1) * SEQ, :ROWS], rows[m * SEQ : (m + 1) * SEQ, ROWS:]
        reals.append(real * twist[0] - imag * twist[1])
        imags.append(real * twist[1] + imag * twist[0])
    z = jnp.concatenate([jnp.concatenate(reals, axis=1), jnp.concatenate(imags, axis=1)], axis=0)
    high = z.astype(BF16)
    final = dot(trail[...], jnp.concatenate([high, high], axis=0))
    if DATA_LOW:
        final += dot(trail[:, : 2 * SEQ], (z - high.astype(F32)).astype(BF16))
    return [final[:, m * ROWS : (m + 1) * ROWS] for m in range(len(pairs))]


def pair_of(spec):
    return spec[:, :ROWS], spec[:, ROWS:]


def rows_of(s, count):
    return pl.ds(pl.multiple_of(s * count, count), count)


def in_steps(body):
    def step(n, carry):
        for k in range(8):
            body(n * 8 + k)
        return carry

    lax.fori_loop(0, SEQ // 8, step, 0)


def owner(seq, half):
    x, z, y = seq // 16, (seq // 4) % 4, seq % 4
    return x * 16 + (z + half * (3 - 2 * z)) * 4 + y


def every_peer(me, half, body, flat=False):
    x, z, y = me // 16, (me // 4) % 4, me % 4
    ys = [(y + d) % 4 for d in (2, 1, 3, 0)]

    def row(dx, other, count):
        base = ((x + dx) % 4) * 16
        owned = other + half * (3 - 2 * other)
        for y_other in ys[:count]:
            body(base + other * 4 + y_other, base + owned * 4 + y_other)

    others = ((z + 2) % 4, z + 1 - 2 * (z % 2), 3 - z, z)

    def plane(dx, carry):
        for other in others:
            row(dx, other, 4)
        return carry

    if flat:
        for dx in range(1, 4):
            plane(dx, 0)
    else:
        lax.fori_loop(1, 4, plane, 0)
    for other in others[:3]:
        row(0, other, 4)
    row(0, z, 3)


def push(src, dst, sems, target):
    copy = pltpu.make_async_remote_copy(
        src_ref=src,
        dst_ref=dst,
        send_sem=sems[0],
        recv_sem=sems[1],
        device_id=target,
        device_id_type=MESH,
    )
    copy.start()
    return copy


def main_kernel(*refs):
    sources, (out, gq, gk, gv, gf, gsk) = refs[:COPIED], refs[COPIED : COPIED + 6]
    copied, loaded = refs[COPIED + 6 : 2 * COPIED + 6], refs[2 * COPIED + 6]
    (
        r, rf, rs, send, send_f, recv, filt, xs, fs, ss, spectra, y, terms, near_in, far_out,
        far_in, out_f, gs, gs_line, sent, got, ready,
    ) = refs[2 * COPIED + 7 :]
    fl, bk, bv, bg, bq, fk, fv, lead, trail, twist, ahead, back, fq, skip = copied
    me, group = lax.axis_index("seq"), lax.axis_index("chan")
    core, half = group % 2, group // 2
    beside, across = 2 * half + (1 - core), 2 * (1 - half) + core
    me_x, me_z, me_y = me // 16, (me // 4) % 4, me % 4
    mirror = {"seq": me_x * 16 + (3 - me_z) * 4 + me_y, "chan": across}
    mine = owner(me, half)
    barrier = pltpu.get_barrier_semaphore()
    loads = [
        pltpu.make_async_copy(sources[n], copied[n], loaded.at[n]) for n in range(COPIED)
    ]
    for load in loads:
        load.start()

    def hello(target, sem=barrier):
        pl.semaphore_signal(sem, inc=1, device_id=target, device_id_type=MESH)

    every_peer(me, half, lambda peer, _: hello({"seq": peer}), True)
    hello({"chan": beside})

    @pl.when(half == 0)
    def _():
        hello(mirror)

    def sems(n):
        return sent.at[n], got.at[n]

    def waiting(ref, n):
        return pltpu.make_async_remote_copy(
            src_ref=ref,
            dst_ref=ref,
            send_sem=sent.at[n],
            recv_sem=got.at[n],
            device_id={"chan": beside},
            device_id_type=MESH,
        )

    def most(ref):
        return ref.at[pl.ds(0, SEQ - 1)]

    def pack(m, left, right):
        for b in range(WIDTH // ROWS):
            cols = slice(b * ROWS, (b + 1) * ROWS)
            xs[m, cols, :] = (left[:, cols].astype(F32) * right[:, cols].astype(F32)).T

        def one(peer):
            send[m, peer] = xs[m, pl.ds(peer, HELD, stride=SEQ), :].astype(BF16)

        in_steps(one)

    def send_signal(m):
        every_peer(
            me,
            half,
            lambda peer, own: push(send.at[m, own], recv.at[m, me], sems(m), {"seq": peer}),
        )
        recv[m, me] = send[m, mine]

    def widen(m):
        waiting(most(recv.at[m]), m).wait_recv()

        def one(s):
            xs[m, rows_of(s, HELD), :] = recv[m, s].astype(F32)

        in_steps(one)

    def send_back(m, held):
        def one(s):
            y[m, s] = xs[held, rows_of(s, HELD), :].astype(BF16)

        in_steps(one)
        every_peer(
            me,
            half,
            lambda peer, _: push(y.at[m, peer], r.at[m, mine], sems(3 + m), {"seq": peer}),
        )
        r[m, mine] = y[m, me]

    loads[0].wait()
    for b in range(QUARTER // ROWS):
        cols = slice(b * ROWS, (b + 1) * ROWS)
        fs[0, cols, :] = fl[:, cols].T

    def filter_rows(peer):
        send_f[peer] = fs[0, pl.ds(peer, PART, stride=SEQ), :].astype(BF16)

    in_steps(filter_rows)
    loads[1].wait()
    loads[2].wait()
    pack(1, bk, bv)

    def pack_loaded(m, left, right, n):
        loads[n].wait()
        loads[n + 1].wait()
        pack(m, left, right)

    pl.semaphore_wait(barrier, SEQ + half)

    @pl.when(half == 1)
    def _():
        hello(mirror, ready)

    every_peer(
        me,
        half,
        lambda peer, own: push(send_f.at[own], filt.at[group, me], sems(6), {"seq": peer}),
    )
    filt[group, me] = send_f[mine]
    send_signal(1)
    pack_loaded(2, bg, bq, 3)
    send_signal(2)
    pack_loaded(0, fk, fv, 5)

    @pl.when(half == 0)
    def _():
        pl.semaphore_wait(ready, 1)

    waiting(most(filt.at[group]), 6).wait_recv()
    whole = filt.at[group]
    moved = [push(whole, whole, sems(7), mirror), push(whole, whole, sems(8), {"chan": beside})]
    send_signal(0)
    for load in loads[7:]:
        load.wait()
    moved[0].wait_recv()
    whole = filt.at[across]
    moved.append(push(whole, whole, sems(9), {"chan": beside}))

    def filter_wide(s):
        for q in range(GROUPS):
            fs[q, pl.ds(s * PART, PART), :] = filt[q, s].astype(F32)

    def column(m, j):
        return xs[m, pl.ds(j, SEQ, stride=HELD), :]

    def put(m, j, value):
        xs[m, pl.ds(j, SEQ, stride=HELD), :] = value

    widen(1)

    def second_ahead(q, carry):
        cols = [column(1, q * PART + k) for k in range(PART)]
        for k, spec in enumerate(forward(cols, lead, twist, ahead)):
            spectra[0, q * PART + k] = spec
        return carry

    lax.fori_loop(0, GROUPS, second_ahead, 0, unroll=UNROLL)
    for copy in moved[1:]:
        copy.wait_recv()
    in_steps(filter_wide)

    def second(q, carry):
        cols = [fs[q, pl.ds(k, SEQ, stride=PART), :] for k in range(PART)]
        pairs = []
        for k, spec in enumerate(forward(cols, lead, twist, ahead)):
            spectra[1, q * PART + k] = spec
            pairs.append(times(pair_of(spec), pair_of(spectra[0, q * PART + k])))
        for k, value in enumerate(inverse(pairs, trail, twist, back)):
            put(3, q * PART + k, value)
        return carry

    lax.fori_loop(0, GROUPS, second, 0, unroll=UNROLL)
    send_back(1, 3)

    widen(2)
    gs[...] = jnp.zeros_like(gs)
    lane = lax.broadcasted_iota(jnp.int32, (1, ROWS), 1)
    scale = 1.0 / math.sqrt(TOTAL)

    def correlate(q, carry):
        cols = [column(2, q * PART + k) for k in range(PART)]
        for k in range(PART):
            part = jnp.sum(cols[k] * column(1, q * PART + k), axis=0, keepdims=True)
            part = jnp.sum(part, axis=1, keepdims=True)
            gs[...] += jnp.where(lane == q * PART + k, part * scale, 0.0)
        spec = forward(cols, lead, twist, ahead)
        pairs = []
        for k in range(PART):
            spectra[2, q * PART + k] = spec[k]
            pairs.append(conj_times(pair_of(spectra[0, q * PART + k]), pair_of(spec[k])))
        for k, value in enumerate(inverse(pairs, trail, twist, back)):
            fs[q, pl.ds(k, SEQ, stride=PART), :] = value
        return carry

    lax.fori_loop(0, GROUPS, correlate, 0, unroll=UNROLL)
    for q in range(GROUPS):
        terms[q] = (fs[q] * scale).astype(BF16)
    swapped = [
        push(terms.at[2 * h + (1 - core)], near_in.at[h], sems(10 + h), {"chan": beside})
        for h in range(2)
    ]

    def through_of(q, carry):
        pairs = []
        for k in range(PART):
            j = q * PART + k
            pairs.append(conj_times(pair_of(spectra[1, j]), pair_of(spectra[2, j])))
        for k, value in enumerate(inverse(pairs, trail, twist, back)):
            put(2, q * PART + k, value)
        return carry

    lax.fori_loop(0, GROUPS, through_of, 0, unroll=UNROLL)
    for copy in swapped:
        copy.wait_recv()
    far_out[...] = (terms[across].astype(F32) + near_in[1 - half].astype(F32)).astype(BF16)
    far = push(far_out, far_in, sems(13), mirror)
    line = [
        push(gs, gs_line.at[mine // 4 % 4], sems(14), {"seq": me_x * 16 + other * 4 + me_y})
        for other in (3 - me_z, (me_z + 2) % 4, me_z + 1 - 2 * (me_z % 2))
    ]
    gs_line[mine // 4 % 4] = gs[...]
    fs[0] = terms[group].astype(F32) + near_in[half].astype(F32)
    send_back(2, 2)

    widen(0)

    def first(q, carry):
        cols = [column(0, q * PART + k) for k in range(PART)]
        spec = forward(cols, lead, twist, ahead)
        pairs = [
            times(pair_of(spectra[1, q * PART + k]), pair_of(spec[k])) for k in range(PART)
        ]
        for k, value in enumerate(inverse(pairs, trail, twist, back)):
            put(0, q * PART + k, value)
        return carry

    lax.fori_loop(0, GROUPS, first, 0, unroll=UNROLL)
    far.wait_recv()
    fs[0] += far_in[...].astype(F32)

    def cut(s):
        out_f[s] = fs[0, pl.ds(s * PART, PART), :].astype(BF16)

    in_steps(cut)
    every_peer(
        me,
        half,
        lambda peer, _: push(out_f.at[peer], rf.at[mine], sems(12), {"seq": peer}),
    )
    rf[mine] = out_f[me]
    whole_line = waiting(gs_line.at[pl.ds(0, 3)], 14)
    whole_line.wait_recv()

    def plane(dx, carry):
        for d in range(4):
            peer = ((me_x + dx) % 4) * 16 + me_z * 4 + (me_y + d) % 4
            push(gs_line, rs.at[me_x * 4 + me_y], sems(15), {"seq": peer})
        return carry

    lax.fori_loop(1, 4, plane, 0)
    for d in range(1, 4):
        peer = me_x * 16 + me_z * 4 + (me_y + d) % 4
        push(gs_line, rs.at[me_x * 4 + me_y], sems(15), {"seq": peer})
    rs[me_x * 4 + me_y] = gs_line[...]
    send_back(0, 0)

    def unpack(m):
        waiting(most(r.at[m]), 3 + m).wait_recv()

        def one(peer):
            xs[m, pl.ds(peer, HELD, stride=SEQ), :] = r[m, peer].astype(F32)

        in_steps(one)

    def product(left, right):
        return (left.astype(F32) * right.astype(F32)).astype(BF16).astype(F32)

    blocks = [slice(b * ROWS, (b + 1) * ROWS) for b in range(WIDTH // ROWS)]
    unpack(1)
    for cols in blocks:
        mixed = xs[1, cols, :].T + skip[:, cols] * product(bk[:, cols], bv[:, cols])
        gq[:, cols] = (bg[:, cols].astype(F32) * mixed).astype(BF16)
    unpack(2)
    for cols in blocks:
        through = xs[2, cols, :].T + skip[:, cols] * product(bg[:, cols], bq[:, cols])
        gk[:, cols] = (through * bv[:, cols].astype(F32)).astype(BF16)
        gv[:, cols] = (through * bk[:, cols].astype(F32)).astype(BF16)
    last = [waiting(most(rf), 12), waiting(rs.at[pl.ds(0, 15)], 15)]
    for copy in last:
        copy.wait_recv()
    ss[...] = jnp.zeros_like(ss)

    def unpack_terms(p):
        fs[0, pl.ds(p, PART, stride=SEQ), :] = rf[p].astype(F32)

    in_steps(unpack_terms)
    for p in range(SEQ):
        ss[p : p + 1, :] = rs[(p // 16) * 4 + p % 4, (p // 4) % 4]
    for cols in blocks[: QUARTER // ROWS]:
        gf[:, cols] = fs[0, cols, :].T
    ss[...] = ss[...].T
    even, odd = ss[pl.ds(0, 8, stride=2), :], ss[pl.ds(1, 8, stride=2), :]
    wide = lax.broadcasted_iota(jnp.int32, (8, ROWS), 1)
    gsk[...] = jnp.where(wide < SEQ, even, pltpu.roll(odd, SEQ, 1))
    unpack(0)
    for cols in blocks:
        mixed = xs[0, cols, :].T + skip[:, cols] * product(fk[:, cols], fv[:, cols])
        out[:, cols] = (fq[:, cols].astype(F32) * mixed).astype(BF16)
    for m in range(3):
        waiting(most(send.at[m]), m).wait_send()
        waiting(most(r.at[m]), 3 + m).wait_send()
    waiting(most(send_f), 6).wait_send()
    for copy in [*moved, *swapped, far, whole_line, *last]:
        copy.wait_send()


def exchange(fl, bk, bv, bg, bq, fk, fv, fq, skip):
    values = (fl, bk, bv, bg, bq, fk, fv, *[jnp.asarray(t) for t in tables()], fq, skip)
    wide = pltpu.VMEM((ROWS, WIDTH), BF16)
    return pl.pallas_call(
        main_kernel,
        out_shape=(
            wide,
            wide,
            wide,
            wide,
            pltpu.VMEM((ROWS, QUARTER), F32),
            pltpu.VMEM((8, ROWS), F32),
        ),
        in_specs=[pl.BlockSpec(memory_space=pltpu.HBM)] * COPIED,
        out_specs=[pl.BlockSpec(memory_space=pltpu.VMEM)] * 6,
        scratch_shapes=[
            *[pltpu.VMEM(v.shape, v.dtype) for v in values],
            pltpu.SemaphoreType.DMA((COPIED,)),
            pltpu.VMEM((3, SEQ, HELD, ROWS), BF16),
            pltpu.VMEM((SEQ, PART, ROWS), BF16),
            pltpu.VMEM((16, 4, 1, ROWS), F32),
            pltpu.VMEM((3, SEQ, HELD, ROWS), BF16),
            pltpu.VMEM((SEQ, PART, ROWS), BF16),
            pltpu.VMEM((3, SEQ, HELD, ROWS), BF16),
            pltpu.VMEM((GROUPS, SEQ, PART, ROWS), BF16),
            pltpu.VMEM((4, WIDTH, ROWS), F32),
            pltpu.VMEM((GROUPS, QUARTER, ROWS), F32),
            pltpu.VMEM((ROWS, ROWS), F32),
            pltpu.VMEM((3, HELD, SEQ, 2 * ROWS), F32),
            pltpu.VMEM((3, SEQ, HELD, ROWS), BF16),
            pltpu.VMEM((GROUPS, QUARTER, ROWS), BF16),
            pltpu.VMEM((2, QUARTER, ROWS), BF16),
            pltpu.VMEM((QUARTER, ROWS), BF16),
            pltpu.VMEM((QUARTER, ROWS), BF16),
            pltpu.VMEM((SEQ, PART, ROWS), BF16),
            pltpu.VMEM((1, ROWS), F32),
            pltpu.VMEM((4, 1, ROWS), F32),
            pltpu.SemaphoreType.DMA((16,)),
            pltpu.SemaphoreType.DMA((16,)),
            pltpu.SemaphoreType.REGULAR,
        ],
        compiler_params=pltpu.CompilerParams(collective_id=0, has_side_effects=True),
    )(*values)


def store_kernel(*refs):
    count = len(refs) // 2
    sems = refs[-1]
    copies = [
        pltpu.make_async_copy(refs[n], refs[count + n], sems.at[n]) for n in range(count)
    ]
    for copy in copies:
        copy.start()
    for copy in copies:
        copy.wait()


def store(values):
    return pl.pallas_call(
        store_kernel,
        out_shape=tuple(jax.ShapeDtypeStruct(v.shape, v.dtype) for v in values),
        in_specs=[pl.BlockSpec(memory_space=pltpu.VMEM)] * len(values),
        out_specs=[pl.BlockSpec(memory_space=pl.ANY)] * len(values),
        scratch_shapes=[pltpu.SemaphoreType.DMA((len(values),))],
    )(*[pltpu.with_memory_space_constraint(v, pltpu.VMEM) for v in values])


def per_device(fwd_q, fwd_k, fwd_v, bwd_q, bwd_k, bwd_v, bwd_grad, filters, skip):
    done = exchange(
        filters, bwd_k, bwd_v, bwd_grad, bwd_q, fwd_k, fwd_v, fwd_q, skip[None, :]
    )
    *wide, skips = store(done)
    return (*wide, skips.reshape(WIDTH))


def solution(mesh):
    both = P("seq", "chan")
    return jax.shard_map(
        per_device,
        mesh=mesh,
        in_specs=(both,) * 8 + (P("chan"),),
        out_specs=(both,) * 5 + (P("chan"),),
        check_vma=False,
    )
```

```python
import functools
import math

import jax
import jax.numpy as jnp
import numpy as np
from jax import lax
from jax.experimental import pallas as pl
from jax.experimental.pallas import tpu as pltpu
from jax.sharding import PartitionSpec as P

MESH = pl.DeviceIdType.MESH
F32 = jnp.float32
BF16 = jnp.bfloat16
ROWS = 128
SEQ = 64
HELD = 16
GROUPS = 4
PART = HELD // GROUPS
TOTAL = ROWS * SEQ
WIDTH = SEQ * HELD
QUARTER = SEQ * PART
UNROLL = 4
COPIED = 14
DATA_LOW = False
TABLE_LOW = True


def halves(table):
    high = np.asarray(table, np.float32).astype(BF16)
    low = (np.asarray(table, np.float64) - high.astype(np.float64)).astype(np.float32).astype(BF16)
    return high, low


@functools.cache
def tables():
    row = np.arange(SEQ)
    lane = np.arange(ROWS)
    coarse = 2 * np.pi * ((row[None, :] * (4 * row[:, None] + 1)) % (4 * SEQ)) / (4 * SEQ)
    lead = np.concatenate([np.cos(coarse), -np.sin(coarse)], axis=0)
    lead = np.concatenate(halves(lead), axis=1)
    trail = np.concatenate([np.cos(coarse.T), -np.sin(coarse.T)], axis=1) / TOTAL
    trail = np.concatenate(halves(trail), axis=1)
    mid = 2 * np.pi * lane[None, :] * (4 * row[:, None] + 1) / (4 * TOTAL)
    twist = np.stack([np.cos(mid), np.sin(mid)]).astype(np.float32)
    fine = 2 * np.pi * ((lane[:, None] * lane[None, :]) % ROWS) / ROWS
    cosine, sine = np.cos(fine), np.sin(fine)
    ahead = np.stack(halves(np.block([[cosine, -sine], [sine, cosine]])))
    back = np.stack(halves(np.block([[cosine, sine], [-sine, cosine]])))
    return lead, trail, twist, ahead, back


def dot(left, right):
    return jnp.dot(left, right, preferred_element_type=F32)


def split_dot(values, table):
    high = values.astype(BF16)
    total = dot(high, table[0])
    if DATA_LOW:
        total += dot((values - high.astype(F32)).astype(BF16), table[0])
    if TABLE_LOW:
        total += dot(high, table[1])
    return total


def times(a, b):
    return a[0] * b[0] - a[1] * b[1], a[0] * b[1] + a[1] * b[0]


def conj_times(a, b):
    return a[0] * b[0] + a[1] * b[1], a[0] * b[1] - a[1] * b[0]


def forward(cols, lead, twist, ahead):
    x = jnp.concatenate(cols, axis=1).astype(BF16)
    front = dot(lead[...], jnp.concatenate([x, x], axis=0))
    rows = []
    for m in range(len(cols)):
        real, imag = front[:SEQ, m * ROWS : (m + 1) * ROWS], front[SEQ:, m * ROWS : (m + 1) * ROWS]
        turned = [real * twist[0] + imag * twist[1], imag * twist[0] - real * twist[1]]
        rows.append(jnp.concatenate(turned, axis=1))
    spec = split_dot(jnp.concatenate(rows, axis=0), ahead)
    return [spec[m * SEQ : (m + 1) * SEQ] for m in range(len(cols))]


def inverse(pairs, trail, twist, back):
    rows = jnp.concatenate([jnp.concatenate(pair, axis=1) for pair in pairs], axis=0)
    rows = split_dot(rows, back)
    reals, imags = [], []
    for m in range(len(pairs)):
        real, imag = rows[m * SEQ : (m + 1) * SEQ, :ROWS], rows[m * SEQ : (m + 1) * SEQ, ROWS:]
        reals.append(real * twist[0] - imag * twist[1])
        imags.append(real * twist[1] + imag * twist[0])
    z = jnp.concatenate([jnp.concatenate(reals, axis=1), jnp.concatenate(imags, axis=1)], axis=0)
    high = z.astype(BF16)
    final = dot(trail[...], jnp.concatenate([high, high], axis=0))
    if DATA_LOW:
        final += dot(trail[:, : 2 * SEQ], (z - high.astype(F32)).astype(BF16))
    return [final[:, m * ROWS : (m + 1) * ROWS] for m in range(len(pairs))]


def pair_of(spec):
    return spec[:, :ROWS], spec[:, ROWS:]


def rows_of(s, count):
    return pl.ds(pl.multiple_of(s * count, count), count)


def in_steps(body, flat=False):
    def step(n, carry):
        for k in range(8):
            body(n * 8 + k)
        return carry

    lax.fori_loop(0, SEQ // 8, step, 0, unroll=SEQ // 8 if flat else 1)


def owner(seq, half):
    x, z, y = seq // 16, (seq // 4) % 4, seq % 4
    return x * 16 + (z + half * (3 - 2 * z)) * 4 + y


def every_peer(me, half, body, flat=False):
    x, z, y = me // 16, (me // 4) % 4, me % 4
    ys = [(y + d) % 4 for d in (2, 1, 3, 0)]

    def row(dx, other, count):
        base = ((x + dx) % 4) * 16
        owned = other + half * (3 - 2 * other)
        for y_other in ys[:count]:
            body(base + other * 4 + y_other, base + owned * 4 + y_other)

    others = ((z + 2) % 4, z + 1 - 2 * (z % 2), 3 - z, z)

    def plane(dx, carry):
        for other in others:
            row(dx, other, 4)
        return carry

    if flat:
        for dx in range(1, 4):
            plane(dx, 0)
    else:
        lax.fori_loop(1, 4, plane, 0)
    for other in others[:3]:
        row(0, other, 4)
    row(0, z, 3)


def push(src, dst, sems, target):
    copy = pltpu.make_async_remote_copy(
        src_ref=src,
        dst_ref=dst,
        send_sem=sems[0],
        recv_sem=sems[1],
        device_id=target,
        device_id_type=MESH,
    )
    copy.start()
    return copy


def main_kernel(*refs):
    sources, (out, gq, gk, gv, gf, gsk) = refs[:COPIED], refs[COPIED : COPIED + 6]
    copied, loaded = refs[COPIED + 6 : 2 * COPIED + 6], refs[2 * COPIED + 6]
    (
        r, rf, rs, send, send_f, recv, filt, xs, fs, ss, spectra, y, terms, near_in, far_out,
        far_in, out_f, gs, gs_line, sent, got, ready,
    ) = refs[2 * COPIED + 7 :]
    fl, bk, bv, bg, bq, fk, fv, lead, trail, twist, ahead, back, fq, skip = copied
    me, group = lax.axis_index("seq"), lax.axis_index("chan")
    core, half = group % 2, group // 2
    beside, across = 2 * half + (1 - core), 2 * (1 - half) + core
    me_x, me_z, me_y = me // 16, (me // 4) % 4, me % 4
    mirror = {"seq": me_x * 16 + (3 - me_z) * 4 + me_y, "chan": across}
    mine = owner(me, half)
    barrier = pltpu.get_barrier_semaphore()
    loads = [
        pltpu.make_async_copy(sources[n], copied[n], loaded.at[n]) for n in range(COPIED)
    ]
    for load in loads:
        load.start()

    def hello(target, sem=barrier):
        pl.semaphore_signal(sem, inc=1, device_id=target, device_id_type=MESH)

    every_peer(me, half, lambda peer, _: hello({"seq": peer}), True)
    hello({"chan": beside})

    @pl.when(half == 0)
    def _():
        hello(mirror)

    def sems(n):
        return sent.at[n], got.at[n]

    def waiting(ref, n):
        return pltpu.make_async_remote_copy(
            src_ref=ref,
            dst_ref=ref,
            send_sem=sent.at[n],
            recv_sem=got.at[n],
            device_id={"chan": beside},
            device_id_type=MESH,
        )

    def most(ref):
        return ref.at[pl.ds(0, SEQ - 1)]

    def pack(m, left, right):
        for b in range(WIDTH // ROWS):
            cols = slice(b * ROWS, (b + 1) * ROWS)
            xs[m, cols, :] = (left[:, cols].astype(F32) * right[:, cols].astype(F32)).T

        def one(peer):
            send[m, peer] = xs[m, pl.ds(peer, HELD, stride=SEQ), :].astype(BF16)

        in_steps(one)

    def send_signal(m):
        every_peer(
            me,
            half,
            lambda peer, own: push(send.at[m, own], recv.at[m, me], sems(m), {"seq": peer}),
        )
        recv[m, me] = send[m, mine]

    def widen(m):
        waiting(most(recv.at[m]), m).wait_recv()

        def one(s):
            xs[m, rows_of(s, HELD), :] = recv[m, s].astype(F32)

        in_steps(one)

    def send_back(m, held):
        def one(s):
            y[m, s] = xs[held, rows_of(s, HELD), :].astype(BF16)

        in_steps(one)
        every_peer(
            me,
            half,
            lambda peer, _: push(y.at[m, peer], r.at[m, mine], sems(3 + m), {"seq": peer}),
        )
        r[m, mine] = y[m, me]

    loads[0].wait()
    for b in range(QUARTER // ROWS):
        cols = slice(b * ROWS, (b + 1) * ROWS)
        fs[0, cols, :] = fl[:, cols].T

    def filter_rows(peer):
        send_f[peer] = fs[0, pl.ds(peer, PART, stride=SEQ), :].astype(BF16)

    in_steps(filter_rows)
    loads[1].wait()
    loads[2].wait()
    pack(1, bk, bv)

    def pack_loaded(m, left, right, n):
        loads[n].wait()
        loads[n + 1].wait()
        pack(m, left, right)

    pl.semaphore_wait(barrier, SEQ + half)

    @pl.when(half == 1)
    def _():
        hello(mirror, ready)

    every_peer(
        me,
        half,
        lambda peer, own: push(send_f.at[own], filt.at[group, me], sems(6), {"seq": peer}),
    )
    filt[group, me] = send_f[mine]
    send_signal(1)
    pack_loaded(2, bg, bq, 3)
    send_signal(2)
    pack_loaded(0, fk, fv, 5)

    @pl.when(half == 0)
    def _():
        pl.semaphore_wait(ready, 1)

    waiting(most(filt.at[group]), 6).wait_recv()
    whole = filt.at[group]
    moved = [push(whole, whole, sems(7), mirror), push(whole, whole, sems(8), {"chan": beside})]
    send_signal(0)
    for load in loads[7:]:
        load.wait()
    moved[0].wait_recv()
    whole = filt.at[across]
    moved.append(push(whole, whole, sems(9), {"chan": beside}))

    def filter_wide(s):
        for q in range(GROUPS):
            fs[q, pl.ds(s * PART, PART), :] = filt[q, s].astype(F32)

    def column(m, j):
        return xs[m, pl.ds(j, SEQ, stride=HELD), :]

    def put(m, j, value):
        xs[m, pl.ds(j, SEQ, stride=HELD), :] = value

    widen(1)

    def second_ahead(q, carry):
        cols = [column(1, q * PART + k) for k in range(PART)]
        for k, spec in enumerate(forward(cols, lead, twist, ahead)):
            spectra[0, q * PART + k] = spec
        return carry

    lax.fori_loop(0, GROUPS, second_ahead, 0, unroll=UNROLL)
    for copy in moved[1:]:
        copy.wait_recv()
    in_steps(filter_wide)

    def second(q, carry):
        cols = [fs[q, pl.ds(k, SEQ, stride=PART), :] for k in range(PART)]
        pairs = []
        for k, spec in enumerate(forward(cols, lead, twist, ahead)):
            spectra[1, q * PART + k] = spec
            pairs.append(times(pair_of(spec), pair_of(spectra[0, q * PART + k])))
        for k, value in enumerate(inverse(pairs, trail, twist, back)):
            put(3, q * PART + k, value)
        return carry

    lax.fori_loop(0, GROUPS, second, 0, unroll=UNROLL)
    send_back(1, 3)

    widen(2)
    gs[...] = jnp.zeros_like(gs)
    lane = lax.broadcasted_iota(jnp.int32, (1, ROWS), 1)
    scale = 1.0 / math.sqrt(TOTAL)

    def correlate(q, carry):
        cols = [column(2, q * PART + k) for k in range(PART)]
        for k in range(PART):
            part = jnp.sum(cols[k] * column(1, q * PART + k), axis=0, keepdims=True)
            part = jnp.sum(part, axis=1, keepdims=True)
            gs[...] += jnp.where(lane == q * PART + k, part * scale, 0.0)
        spec = forward(cols, lead, twist, ahead)
        pairs = []
        for k in range(PART):
            spectra[2, q * PART + k] = spec[k]
            pairs.append(conj_times(pair_of(spectra[0, q * PART + k]), pair_of(spec[k])))
        for k, value in enumerate(inverse(pairs, trail, twist, back)):
            fs[q, pl.ds(k, SEQ, stride=PART), :] = value
        return carry

    lax.fori_loop(0, GROUPS, correlate, 0, unroll=UNROLL)
    for q in range(GROUPS):
        terms[q] = (fs[q] * scale).astype(BF16)
    swapped = [
        push(terms.at[2 * h + (1 - core)], near_in.at[h], sems(10 + h), {"chan": beside})
        for h in range(2)
    ]

    def through_of(q, carry):
        pairs = []
        for k in range(PART):
            j = q * PART + k
            pairs.append(conj_times(pair_of(spectra[1, j]), pair_of(spectra[2, j])))
        for k, value in enumerate(inverse(pairs, trail, twist, back)):
            put(2, q * PART + k, value)
        return carry

    lax.fori_loop(0, GROUPS, through_of, 0, unroll=UNROLL)
    for copy in swapped:
        copy.wait_recv()
    far_out[...] = (terms[across].astype(F32) + near_in[1 - half].astype(F32)).astype(BF16)
    far = push(far_out, far_in, sems(13), mirror)
    line = [
        push(gs, gs_line.at[mine // 4 % 4], sems(14), {"seq": me_x * 16 + other * 4 + me_y})
        for other in (3 - me_z, (me_z + 2) % 4, me_z + 1 - 2 * (me_z % 2))
    ]
    gs_line[mine // 4 % 4] = gs[...]
    fs[0] = terms[group].astype(F32) + near_in[half].astype(F32)
    send_back(2, 2)

    widen(0)

    def first(q, carry):
        cols = [column(0, q * PART + k) for k in range(PART)]
        spec = forward(cols, lead, twist, ahead)
        pairs = [
            times(pair_of(spectra[1, q * PART + k]), pair_of(spec[k])) for k in range(PART)
        ]
        for k, value in enumerate(inverse(pairs, trail, twist, back)):
            put(0, q * PART + k, value)
        return carry

    lax.fori_loop(0, GROUPS, first, 0, unroll=UNROLL)
    far.wait_recv()
    fs[0] += far_in[...].astype(F32)

    def cut(s):
        out_f[s] = fs[0, pl.ds(s * PART, PART), :].astype(BF16)

    in_steps(cut)
    every_peer(
        me,
        half,
        lambda peer, _: push(out_f.at[peer], rf.at[mine], sems(12), {"seq": peer}),
    )
    rf[mine] = out_f[me]
    whole_line = waiting(gs_line.at[pl.ds(0, 3)], 14)
    whole_line.wait_recv()

    def plane(dx, carry):
        for d in range(4):
            peer = ((me_x + dx) % 4) * 16 + me_z * 4 + (me_y + d) % 4
            push(gs_line, rs.at[me_x * 4 + me_y], sems(15), {"seq": peer})
        return carry

    lax.fori_loop(1, 4, plane, 0)
    for d in range(1, 4):
        peer = me_x * 16 + me_z * 4 + (me_y + d) % 4
        push(gs_line, rs.at[me_x * 4 + me_y], sems(15), {"seq": peer})
    rs[me_x * 4 + me_y] = gs_line[...]
    send_back(0, 0)

    def unpack(m, flat=False):
        waiting(most(r.at[m]), 3 + m).wait_recv()

        def one(peer):
            xs[m, pl.ds(peer, HELD, stride=SEQ), :] = r[m, peer].astype(F32)

        in_steps(one, flat)

    def product(left, right):
        return (left.astype(F32) * right.astype(F32)).astype(BF16).astype(F32)

    blocks = [slice(b * ROWS, (b + 1) * ROWS) for b in range(WIDTH // ROWS)]
    unpack(1)
    for cols in blocks:
        mixed = xs[1, cols, :].T + skip[:, cols] * product(bk[:, cols], bv[:, cols])
        gq[:, cols] = (bg[:, cols].astype(F32) * mixed).astype(BF16)
    unpack(2)
    for cols in blocks:
        through = xs[2, cols, :].T + skip[:, cols] * product(bg[:, cols], bq[:, cols])
        gk[:, cols] = (through * bv[:, cols].astype(F32)).astype(BF16)
        gv[:, cols] = (through * bk[:, cols].astype(F32)).astype(BF16)
    last = [waiting(most(rf), 12), waiting(rs.at[pl.ds(0, 15)], 15)]
    for copy in last:
        copy.wait_recv()
    ss[...] = jnp.zeros_like(ss)

    def unpack_terms(p):
        fs[0, pl.ds(p, PART, stride=SEQ), :] = rf[p].astype(F32)

    in_steps(unpack_terms)
    for p in range(SEQ):
        ss[p : p + 1, :] = rs[(p // 16) * 4 + p % 4, (p // 4) % 4]
    for cols in blocks[: QUARTER // ROWS]:
        gf[:, cols] = fs[0, cols, :].T
    ss[...] = ss[...].T
    even, odd = ss[pl.ds(0, 8, stride=2), :], ss[pl.ds(1, 8, stride=2), :]
    wide = lax.broadcasted_iota(jnp.int32, (8, ROWS), 1)
    gsk[...] = jnp.where(wide < SEQ, even, pltpu.roll(odd, SEQ, 1))
    for cols in blocks:
        xs[3, cols, :] = skip[:, cols] * product(fk[:, cols], fv[:, cols])
    unpack(0, True)
    for cols in blocks:
        mixed = xs[0, cols, :].T + xs[3, cols, :]
        out[:, cols] = (fq[:, cols].astype(F32) * mixed).astype(BF16)
    for m in range(3):
        waiting(most(send.at[m]), m).wait_send()
        waiting(most(r.at[m]), 3 + m).wait_send()
    waiting(most(send_f), 6).wait_send()
    for copy in [*moved, *swapped, far, whole_line, *last]:
        copy.wait_send()


def exchange(fl, bk, bv, bg, bq, fk, fv, fq, skip):
    values = (fl, bk, bv, bg, bq, fk, fv, *[jnp.asarray(t) for t in tables()], fq, skip)
    wide = pltpu.VMEM((ROWS, WIDTH), BF16)
    return pl.pallas_call(
        main_kernel,
        out_shape=(
            wide,
            wide,
            wide,
            wide,
            pltpu.VMEM((ROWS, QUARTER), F32),
            pltpu.VMEM((8, ROWS), F32),
        ),
        in_specs=[pl.BlockSpec(memory_space=pltpu.HBM)] * COPIED,
        out_specs=[pl.BlockSpec(memory_space=pltpu.VMEM)] * 6,
        scratch_shapes=[
            *[pltpu.VMEM(v.shape, v.dtype) for v in values],
            pltpu.SemaphoreType.DMA((COPIED,)),
            pltpu.VMEM((3, SEQ, HELD, ROWS), BF16),
            pltpu.VMEM((SEQ, PART, ROWS), BF16),
            pltpu.VMEM((16, 4, 1, ROWS), F32),
            pltpu.VMEM((3, SEQ, HELD, ROWS), BF16),
            pltpu.VMEM((SEQ, PART, ROWS), BF16),
            pltpu.VMEM((3, SEQ, HELD, ROWS), BF16),
            pltpu.VMEM((GROUPS, SEQ, PART, ROWS), BF16),
            pltpu.VMEM((4, WIDTH, ROWS), F32),
            pltpu.VMEM((GROUPS, QUARTER, ROWS), F32),
            pltpu.VMEM((ROWS, ROWS), F32),
            pltpu.VMEM((3, HELD, SEQ, 2 * ROWS), F32),
            pltpu.VMEM((3, SEQ, HELD, ROWS), BF16),
            pltpu.VMEM((GROUPS, QUARTER, ROWS), BF16),
            pltpu.VMEM((2, QUARTER, ROWS), BF16),
            pltpu.VMEM((QUARTER, ROWS), BF16),
            pltpu.VMEM((QUARTER, ROWS), BF16),
            pltpu.VMEM((SEQ, PART, ROWS), BF16),
            pltpu.VMEM((1, ROWS), F32),
            pltpu.VMEM((4, 1, ROWS), F32),
            pltpu.SemaphoreType.DMA((16,)),
            pltpu.SemaphoreType.DMA((16,)),
            pltpu.SemaphoreType.REGULAR,
        ],
        compiler_params=pltpu.CompilerParams(collective_id=0, has_side_effects=True),
    )(*values)


def store_kernel(*refs):
    count = len(refs) // 2
    sems = refs[-1]
    copies = [
        pltpu.make_async_copy(refs[n], refs[count + n], sems.at[n]) for n in range(count)
    ]
    for copy in copies:
        copy.start()
    for copy in copies:
        copy.wait()


def store(values):
    return pl.pallas_call(
        store_kernel,
        out_shape=tuple(jax.ShapeDtypeStruct(v.shape, v.dtype) for v in values),
        in_specs=[pl.BlockSpec(memory_space=pltpu.VMEM)] * len(values),
        out_specs=[pl.BlockSpec(memory_space=pl.ANY)] * len(values),
        scratch_shapes=[pltpu.SemaphoreType.DMA((len(values),))],
    )(*[pltpu.with_memory_space_constraint(v, pltpu.VMEM) for v in values])


def per_device(fwd_q, fwd_k, fwd_v, bwd_q, bwd_k, bwd_v, bwd_grad, filters, skip):
    done = exchange(
        filters, bwd_k, bwd_v, bwd_grad, bwd_q, fwd_k, fwd_v, fwd_q, skip[None, :]
    )
    *wide, skips = store(done)
    return (*wide, skips.reshape(WIDTH))


def solution(mesh):
    both = P("seq", "chan")
    return jax.shard_map(
        per_device,
        mesh=mesh,
        in_specs=(both,) * 8 + (P("chan"),),
        out_specs=(both,) * 5 + (P("chan"),),
        check_vma=False,
    )
```
